512 devices in a mesh: pair: 16 (over y, x), side: 2 (over z_hi), blk: 16 (over z_lo, core).
Axes of the slice: x: 4, y: 4, z: 16 (z_hi: 2, z_lo: 8; z = z_hi * 8 + z_lo), core: 2. Of those that a mesh axis runs over, the one named last changes fastest.
Arguments:
- intersect: float32 [65536, 768], P(('pair', 'side', 'blk')), parts along dimension 0, may hold values from -0.1 to 1.7, as said below
- half_factors: float32 [65536, 384], P(('pair', 'side', 'blk')), parts along dimension 0, may hold values from -0.03 to 1.35, as said below
- z_pattern: int32 [512, 6], P(('pair', 'side', 'blk')), parts along dimension 0, may hold values 0 or 1
Outputs:
- refined_factor: float32 [65536, 768], P(('pair', 'side', 'blk')), parts along dimension 0
The draws below stay inside these ranges and needn't reach their ends.
There are 16 independent parts, one for each index of `pair`. The reference program is written for one: setup_inputs(seed, part) draws one part's arguments, and reference() takes and returns one part's arrays. A program takes and returns all parts, laid end to end along the dimension named above; each array names one. Nothing has to cross between parts.
Inputs may be any that keep to these rules, and one draw needn't show every extreme that they name: As a whole windowed matrix, intersect is symmetric: S[a, b] = S[b, a]. `half_factors`: entries of the other half and outside the grid of blocks are absent or zero. `z_pattern`: 1 keeps a tile of the factor, 0 drops it; diagonal tiles are kept whatever it says.
All inputs are finite; a program needn't handle non-finite values. No bound on the sum of `z_pattern` on one device may be relied on, other than what follows from the above.
Results may differ from the reference program's by a relative error of at most 0.0001.
Values sent between devices are 32-bit elements; how exact they have to be, the bound alone decides.
A program may use at most 64 MiB of HBM per device.

```python
import jax
import jax.numpy as jnp
from jax import lax

TILE = 128
TILES_DEV = 1
ITERS = 2
TILE_ROWS = 32
N_BLK = 16


def diag_values(key):
    rows = TILE * TILES_DEV
    draw_key = jax.random.fold_in(key, 11)
    fraction = jax.random.uniform(draw_key, (2, N_BLK, rows), jnp.float32)
    return 0.7 * jnp.exp(fraction * jnp.log(1.5 / 0.7))


def block_inside(blocks):
    column = jnp.arange(blocks)[:, None] + jnp.arange(3)[None, :] - 1
    return ((column >= 0) & (column < blocks)).astype(jnp.float32)


def window_transpose(field):
    empty = jnp.zeros_like(field[:, :1, :, 0])
    pieces = []
    for slot in range(3):
        source = field[:, :, :, 2 - slot]
        if slot == 2:
            source = jnp.concatenate((source[:, 1:], empty), axis=1)
        if slot == 0:
            source = jnp.concatenate((empty, source[:, :-1]), axis=1)
        pieces.append(jnp.transpose(source, (3, 1, 4, 0, 2)))
    return jnp.stack(pieces, axis=3)


def draw_intersect(key, part):
    rows = TILE * TILES_DEV
    blocks = N_BLK
    shape = (2, blocks, rows, 3, 2, rows)
    sigma = 0.012
    noise_key = jax.random.fold_in(key, 3)
    raw = jnp.clip(jax.random.normal(noise_key, shape, jnp.float32), -6.0, 6.0) * sigma
    tile_key = jax.random.fold_in(key, 5)
    present = jax.random.bernoulli(tile_key, 0.75, (2, blocks, TILES_DEV, 3, 2, TILES_DEV)).astype(jnp.float32)
    present = jnp.repeat(jnp.repeat(present, TILE, axis=2), TILE, axis=5)
    inside = block_inside(blocks)[None, :, None, :, None, None]
    coupling = raw * present * inside
    symmetric = 0.5 * (coupling + window_transpose(coupling))
    eye_side = jnp.eye(2, dtype=jnp.float32)
    eye_rows = jnp.eye(rows, dtype=jnp.float32)
    middle = (jnp.arange(3) == 1).astype(jnp.float32)
    diagonal = diag_values(key)[:, :, :, None, None, None] * eye_side[:, None, None, None, :, None] * eye_rows[None, None, :, None, None, :] * middle[None, None, None, :, None, None]
    return (symmetric + diagonal).reshape(2 * blocks * rows, 6 * rows)


def draw_half_factors(key, part):
    rows = TILE * TILES_DEV
    blocks = N_BLK
    shape = (2, blocks, rows, 3, rows)
    sigma = 0.004
    noise_key = jax.random.fold_in(key, 17)
    raw = jnp.clip(jax.random.normal(noise_key, shape, jnp.float32), -6.0, 6.0) * sigma
    inside = block_inside(blocks)[None, :, None, :, None]
    eye_rows = jnp.eye(rows, dtype=jnp.float32)
    middle = (jnp.arange(3) == 1).astype(jnp.float32)
    scales = 1.0 / jnp.sqrt(diag_values(key))
    diagonal = scales[:, :, :, None, None] * eye_rows[None, None, :, None, :] * middle[None, None, None, :, None]
    return (raw * inside + diagonal).reshape(2 * blocks * rows, 3 * rows)


def set_ends(array, rng, low, top_value):
    index_at = [jax.random.randint(jax.random.fold_in(rng, axis), (), 0, length) for axis, length in enumerate(array.shape)]
    main_axis = array.shape.index(max(array.shape))
    next_to = index_at[:main_axis] + [(index_at[main_axis] + 1) % array.shape[main_axis]] + index_at[main_axis + 1:]
    return array.at[tuple(index_at)].set(low).at[tuple(next_to)].set(top_value)


def setup_inputs(seed: int = 0, part: int = 0) -> dict:
    seeds = jax.random.split(jax.random.key(seed), 4)
    own_keys = jax.random.split(jax.random.fold_in(seeds[3], part), 4)
    return {
        "intersect": draw_intersect(jax.random.fold_in(jax.random.fold_in(seeds[3], part), 71), part),
        "half_factors": draw_half_factors(jax.random.fold_in(jax.random.fold_in(seeds[3], part), 71), part),
        "z_pattern": set_ends((jax.random.randint(own_keys[2], (TILE_ROWS, 6 * TILES_DEV), 0, 4) < 3).astype(jnp.int32), jax.random.fold_in(own_keys[2], 1), 0, 1),
    }


def shift_blocks(field, offset):
    empty = jnp.zeros_like(field[:, :1])
    if offset == 1:
        return jnp.concatenate((field[:, 1:], empty), axis=1)
    if offset == -1:
        return jnp.concatenate((empty, field[:, :-1]), axis=1)
    return field


def shift_slots(term, slot):
    empty = jnp.zeros_like(term[:, :, :, :1])
    if slot == 0:
        return jnp.concatenate((term[:, :, :, 1:], empty), axis=3)
    if slot == 2:
        return jnp.concatenate((empty, term[:, :, :, :2]), axis=3)
    return term


def window_product(left, right):
    total = jnp.zeros_like(right)
    for slot in range(3):
        nearby = shift_blocks(right, slot - 1)
        term = jnp.einsum("sbixk,xbkdyj->sbidyj", left[:, :, :, slot], nearby, precision=lax.Precision.HIGHEST)
        total = total + shift_slots(term, slot)
    return total


def window_cross(factor, image):
    total = jnp.zeros_like(image)
    for slot in range(3):
        near_factor = shift_blocks(factor, slot - 1)
        near_image = shift_blocks(image, slot - 1)
        term = jnp.einsum("xbksi,xbkdyj->sbidyj", near_factor[:, :, :, 2 - slot], near_image, precision=lax.Precision.HIGHEST)
        total = total + shift_slots(term, slot)
    return total


def reference(intersect, half_factors, z_pattern):
    blocks = N_BLK
    rows = intersect.shape[1] // 6
    tiles = z_pattern.shape[1] // 6
    tile = rows // tiles
    intersect_win = intersect.reshape(2, blocks, rows, 3, 2, rows)
    half_win = half_factors.reshape(2, blocks, rows, 3, rows)
    eye_side = jnp.eye(2, dtype=jnp.float32)
    eye_rows = jnp.eye(rows, dtype=jnp.float32)
    middle = (jnp.arange(3) == 1).astype(jnp.float32)
    identity = eye_side[:, None, None, None, :, None] * eye_rows[None, None, :, None, None, :] * middle[None, None, None, :, None, None]
    grid = z_pattern.reshape(2, blocks, tiles, 3, 2, tiles)
    halves = jnp.arange(2)
    tile_ids = jnp.arange(tiles)
    diagonal = (halves[:, None, None, None, None, None] == halves[None, None, None, None, :, None]) & (tile_ids[None, None, :, None, None, None] == tile_ids[None, None, None, None, None, :]) & (jnp.arange(3)[None, None, None, :, None, None] == 1)
    kept = jnp.maximum(grid, diagonal.astype(jnp.int32)).astype(jnp.float32)
    wide = jnp.broadcast_to(kept[:, :, :, None, :, :, :, None], (2, blocks, tiles, tile, 3, 2, tiles, tile))
    keep = wide.reshape(2, blocks, rows, 3, 2, rows)
    factor = half_win[:, :, :, :, None, :] * eye_side[:, None, None, None, :, None]
    for step in range(ITERS):
        image = window_product(intersect_win, factor)
        delta = identity - window_cross(factor, image)
        first = window_product(factor, delta)
        second = window_product(first, delta)
        factor = keep * (factor + 0.5 * first + 0.375 * second)
    return factor.reshape(2 * blocks * rows, 6 * rows)
```

```python
import jax
import jax.numpy as jnp
from jax import lax
from jax.experimental import pallas as pl
from jax.experimental.pallas import tpu as pltpu
from jax.sharding import PartitionSpec as P

ITERS = 2
MESH = pl.DeviceIdType.MESH
F32 = jnp.float32
BF16 = jnp.bfloat16
B = 256
SPAN = {0: (0, 512), 1: (0, 768), 2: (256, 768)}


def split(value):
    high = value.astype(BF16)
    low = (value - high.astype(F32)).astype(BF16)
    return high, low


def dot3(left, right, nt):
    dims = (((1,), (1 if nt else 0,)), ((), ()))

    def one(x, y):
        return lax.dot_general(x, y, dims, preferred_element_type=F32)

    return one(left[0], right[0]) + one(left[0], right[1]) + one(left[1], right[0])


def make_kernel(n_blk, tile):
    own = pl.ds(B, tile)
    other = pl.ds(B + tile, tile)
    both = pl.ds(B, B)

    def col(slot, half):
        return pl.ds(slot * B + half * tile, tile)

    def cols(slot):
        return pl.ds(slot * B, B)

    def kernel(s_hbm, h_hbm, zp_ref, out_ref, sn, z0, z1, d0, d1, so_dn, so_up, sx_dn, kbuf, kx,
               s_hi, s_lo, z_hi, z_lo, d_hi, d_lo, lsem, ssem, rsem):
        side = lax.axis_index("side")
        blk = lax.axis_index("blk")
        partner = {"side": 1 - side}
        up = {"blk": blk + 1}
        dn = {"blk": blk - 1}
        has_up = blk < n_blk - 1
        has_dn = blk > 0

        barrier = pltpu.get_barrier_semaphore()
        pl.semaphore_signal(barrier, inc=1, device_id=partner, device_id_type=MESH)

        @pl.when(has_up)
        def _():
            pl.semaphore_signal(barrier, inc=1, device_id=up, device_id_type=MESH)

        @pl.when(has_dn)
        def _():
            pl.semaphore_signal(barrier, inc=1, device_id=dn, device_id_type=MESH)

        loads = []
        for e in range(3):
            loads.append(pltpu.make_async_copy(h_hbm.at[:, pl.ds(e * tile, tile)], z0.at[own, col(e, 0)], lsem.at[6 + e]))
        for e in range(3):
            for g in range(2):
                half = side if g == 0 else 1 - side
                src = s_hbm.at[:, pl.ds(pl.multiple_of((2 * e + half) * tile, tile), tile)]
                loads.append(pltpu.make_async_copy(src, sn.at[own, col(e, g)], lsem.at[2 * e + g]))
        for load in loads:
            load.start()

        keep_own = [zp_ref[0, 2 * e + (side if g == 0 else 1 - side)].astype(F32) for e in range(3) for g in range(2)]
        row_id = lax.broadcasted_iota(jnp.int32, (8, tile), 0)
        packed = jnp.zeros((8, tile), F32)
        for r in range(6):
            packed = jnp.where(row_id == r, keep_own[r], packed)
        kbuf[...] = packed

        zero = jnp.zeros((tile, tile), F32)
        for e in range(3):
            z0[own, col(e, 1)] = zero
            z0[other, col(e, 0)] = zero
        for e in (0, 1):
            z0[pl.ds(0, tile), col(e, 1)] = zero
            z0[pl.ds(tile, tile), col(e, 0)] = zero
            z0[pl.ds(2 * B, tile), col(e + 1, 1)] = zero
            z0[pl.ds(2 * B + tile, tile), col(e + 1, 0)] = zero

        @pl.when(jnp.logical_not(has_dn))
        def _():
            for e in (0, 1):
                z0[pl.ds(0, tile), col(e, 0)] = zero
                z0[pl.ds(tile, tile), col(e, 1)] = zero
                for ref in (z1, d0, d1):
                    ref[pl.ds(0, B), cols(e)] = jnp.zeros((B, B), F32)
            sn[pl.ds(0, tile), pl.ds(0, B)] = jnp.zeros((tile, B), F32)
            sn[pl.ds(tile, tile), pl.ds(tile, tile)] = zero
            so_dn[...] = zero
            sx_dn[...] = zero

        @pl.when(jnp.logical_not(has_up))
        def _():
            for e in (1, 2):
                z0[pl.ds(2 * B, tile), col(e, 0)] = zero
                z0[pl.ds(2 * B + tile, tile), col(e, 1)] = zero
                for ref in (z1, d0, d1):
                    ref[pl.ds(2 * B, B), cols(e)] = jnp.zeros((B, B), F32)
            sn[pl.ds(2 * B, tile), pl.ds(2 * B, B)] = jnp.zeros((tile, B), F32)
            sn[pl.ds(2 * B + tile, tile), pl.ds(2 * B + tile, tile)] = zero
            so_up[...] = zero

        inner = jnp.logical_and(has_up, has_dn)

        @pl.when(inner)
        def _():
            pl.semaphore_wait(barrier, 3)

        @pl.when(jnp.logical_not(inner))
        def _():
            pl.semaphore_wait(barrier, 2)

        used = []

        def remote(src, dst, where):
            i = len(used)
            copy = pltpu.make_async_remote_copy(
                src_ref=src, dst_ref=dst, send_sem=ssem.at[i], recv_sem=rsem.at[i],
                device_id={"x": partner, "u": up, "d": dn}[where], device_id_type=MESH)
            used.append((copy, where))
            return copy

        def start(ups, dns):
            if ups:
                @pl.when(has_up)
                def _():
                    for c in ups:
                        c.start()
            if dns:
                @pl.when(has_dn)
                def _():
                    for c in dns:
                        c.start()

        def receive(ups, dns):
            if ups:
                @pl.when(has_dn)
                def _():
                    for c in ups:
                        c.wait_recv()
            if dns:
                @pl.when(has_up)
                def _():
                    for c in dns:
                        c.wait_recv()

        for load in loads:
            load.wait()
        x_z = [remote(z0.at[own, col(e, 0)], z0.at[other, col(e, 1)], "x") for e in range(3)]
        x_s1 = remote(sn.at[own, col(1, 0)], sn.at[other, col(1, 1)], "x")
        x_s2 = remote(sn.at[own, col(2, 0)], sn.at[other, col(2, 1)], "x")
        x_k = remote(kbuf, kx, "x")
        for c in (x_z[1], x_z[0], x_z[2], x_s1, x_s2, x_k):
            c.start()

        lo, hi = pl.ds(0, tile), pl.ds(tile, tile)
        top, tox = pl.ds(2 * B, tile), pl.ds(2 * B + tile, tile)
        u_own = [
            remote(z0.at[own, col(1, 0)], z0.at[lo, col(0, 0)], "u"),
            remote(z0.at[own, col(2, 0)], z0.at[lo, col(1, 0)], "u"),
            remote(sn.at[own, cols(1)], sn.at[lo, cols(0)], "u"),
            remote(sn.at[own, col(2, 1)], so_dn, "u"),
        ]
        d_own = [
            remote(z0.at[own, col(0, 0)], z0.at[top, col(1, 0)], "d"),
            remote(z0.at[own, col(1, 0)], z0.at[top, col(2, 0)], "d"),
            remote(sn.at[own, cols(1)], sn.at[top, cols(2)], "d"),
            remote(sn.at[own, col(0, 1)], so_up, "d"),
        ]
        start(u_own, d_own)

        x_z[1].wait_recv()
        u_z1 = remote(z0.at[other, col(1, 1)], z0.at[hi, col(0, 1)], "u")
        d_z1 = remote(z0.at[other, col(1, 1)], z0.at[tox, col(2, 1)], "d")
        start([u_z1], [d_z1])
        x_z[0].wait_recv()
        d_z0 = remote(z0.at[other, col(0, 1)], z0.at[tox, col(1, 1)], "d")
        start([], [d_z0])
        x_z[2].wait_recv()
        u_z2 = remote(z0.at[other, col(2, 1)], z0.at[hi, col(1, 1)], "u")
        start([u_z2], [])
        x_s1.wait_recv()
        u_s1 = remote(sn.at[other, col(1, 1)], sn.at[hi, col(0, 1)], "u")
        d_s1 = remote(sn.at[other, col(1, 1)], sn.at[tox, col(2, 1)], "d")
        start([u_s1], [d_s1])
        x_s2.wait_recv()
        u_s2 = remote(sn.at[other, col(2, 1)], sx_dn, "u")
        start([u_s2], [])

        sn[other, col(1, 0)] = sn[own, col(1, 1)].T
        receive(u_own, d_own)
        sn[other, col(0, 0)] = so_dn[...].T
        sn[other, col(2, 0)] = so_up[...].T
        sn[hi, col(0, 0)] = sn[lo, col(0, 1)].T
        sn[tox, col(2, 0)] = sn[top, col(2, 1)].T
        receive([u_z1, u_z2, u_s1, u_s2], [d_z0, d_z1, d_s1])
        sn[other, col(0, 1)] = sx_dn[...].T
        x_k.wait_recv()

        def store_split(ref, rows, slots, refs):
            for slot in slots:
                high, low = split(ref[rows, cols(slot)])
                refs[0][rows, cols(slot)] = high
                refs[1][rows, cols(slot)] = low

        row0, row1, row2 = pl.ds(0, B), both, pl.ds(2 * B, B)

        def pick(refs, rows, columns):
            return refs[0][rows, columns], refs[1][rows, columns]

        def span(slot):
            low, high = SPAN[slot]
            return pl.ds(low, high - low)

        def cut(pair, slot):
            low, high = SPAN[slot]
            return pair[0][:, low:high], pair[1][:, low:high]

        s_refs, z_refs, d_refs = (s_hi, s_lo), (z_hi, z_lo), (d_hi, d_lo)
        store_split(sn, row0, (0,), s_refs)
        store_split(sn, row1, (0, 1, 2), s_refs)
        store_split(sn, row2, (2,), s_refs)

        eye = (lax.broadcasted_iota(jnp.int32, (B, B), 0) == lax.broadcasted_iota(jnp.int32, (B, B), 1)).astype(F32)

        for step in range(ITERS):
            last = step == ITERS - 1
            z, d = (z0, d0) if step == 0 else (z1, d1)
            store_split(z, row0, (0, 1), z_refs)
            store_split(z, row1, (0, 1, 2), z_refs)
            store_split(z, row2, (1, 2), z_refs)
            z_t = split(jnp.concatenate([z[pl.ds(k * B, B), cols(1)].T for k in range(3)], axis=1))
            t_parts = [
                dot3(cut(z_t, 0), pick(s_refs, span(0), cols(0)), False),
                dot3(z_t, pick(s_refs, row1, span(1)), True),
                dot3(cut(z_t, 2), pick(s_refs, span(2), cols(2)), False),
            ]
            t = split(jnp.concatenate(t_parts, axis=1))
            d[row1, cols(1)] = eye - dot3(t, pick(z_refs, span(1), cols(1)), False)
            ups = [remote(d.at[row1, cols(1)], d.at[row0, cols(0)], "u")]
            dns = [remote(d.at[row1, cols(1)], d.at[row2, cols(2)], "d")]
            start(ups, dns)
            d[row1, cols(2)] = -dot3(cut(t, 2), pick(z_refs, span(2), cols(2)), False)
            ups.append(remote(d.at[row1, cols(2)], d.at[row0, cols(1)], "u"))
            start(ups[1:], [])
            d[row1, cols(0)] = -dot3(cut(t, 0), pick(z_refs, span(0), cols(0)), False)
            dns.append(remote(d.at[row1, cols(0)], d.at[row2, cols(1)], "d"))
            start([], dns[1:])

            rows = tile if last else B
            mine = pl.ds(B, rows)
            left = pick(z_refs, mine, span(1))
            store_split(d, row1, (0, 1, 2), d_refs)
            f_mid = dot3(left, pick(d_refs, row1, span(1)), True)
            receive(ups, dns)
            store_split(d, row0, (0, 1), d_refs)
            store_split(d, row2, (1, 2), d_refs)

            def apply(pair, slot):
                return dot3(cut(pair, slot), pick(d_refs, pl.ds(slot * B, B), span(slot)), True)

            first = [apply(left, 0), f_mid, apply(left, 2)]
            pair = split(jnp.concatenate(first, axis=1))
            sends = []
            for slot in (1, 2, 0):
                second = apply(pair, slot)
                value = z[mine, cols(slot)] + 0.5 * first[slot] + 0.375 * second
                for g in range(2):
                    part = value[:tile, g * tile:(g + 1) * tile]
                    if not (slot == 1 and g == 0):
                        part = part * keep_own[2 * slot + g]
                    if last:
                        half = side if g == 0 else 1 - side
                        out_ref[:, pl.ds(pl.multiple_of((2 * slot + half) * tile, tile), tile)] = part
                    else:
                        z1[own, col(slot, g)] = part
                        part = value[tile:, g * tile:(g + 1) * tile]
                        if not (slot == 1 and g == 1):
                            r = 2 * slot + 1 - g
                            part = part * kx[r:r + 1, :]
                        z1[other, col(slot, g)] = part
                if not last:
                    ups = [] if slot == 0 else [remote(z1.at[row1, cols(slot)], z1.at[row0, cols(slot - 1)], "u")]
                    dns = [] if slot == 2 else [remote(z1.at[row1, cols(slot)], z1.at[row2, cols(slot + 1)], "d")]
                    start(ups, dns)
                    sends.append((ups, dns))
            for ups, dns in sends:
                receive(ups, dns)

        for c, where in used:
            if where == "x":
                c.wait_send()

        @pl.when(has_up)
        def _():
            for c, where in used:
                if where == "u":
                    c.wait_send()

        @pl.when(has_dn)
        def _():
            for c, where in used:
                if where == "d":
                    c.wait_send()

    return kernel


def solution(mesh):
    n_blk = mesh.shape["blk"]

    def per_device(intersect, half_factors, z_pattern):
        tile = intersect.shape[0]
        near = pltpu.VMEM((3 * B, 3 * B), F32)
        half = pltpu.VMEM((3 * B, 3 * B), BF16)
        block = pltpu.VMEM((tile, tile), F32)
        return pl.pallas_call(
            make_kernel(n_blk, tile),
            out_shape=jax.ShapeDtypeStruct(intersect.shape, F32),
            in_specs=[
                pl.BlockSpec(memory_space=pl.ANY),
                pl.BlockSpec(memory_space=pl.ANY),
                pl.BlockSpec(memory_space=pltpu.SMEM),
            ],
            out_specs=pl.BlockSpec(memory_space=pltpu.VMEM),
            scratch_shapes=[near] * 5 + [block] * 3 + [pltpu.VMEM((8, tile), F32)] * 2 + [half] * 6

            + [pltpu.SemaphoreType.DMA((9,)), pltpu.SemaphoreType.DMA((48,)), pltpu.SemaphoreType.DMA((48,))],
            compiler_params=pltpu.CompilerParams(
                collective_id=0, has_side_effects=True, vmem_limit_bytes=48 * 1024 * 1024),
            name="merge",
        )(intersect, half_factors, z_pattern)

    spec = P(("pair", "side", "blk"), None)
    return jax.shard_map(per_device, mesh=mesh, in_specs=(spec,) * 3, out_specs=spec, check_vma=False)
```

```python
import jax
import jax.numpy as jnp
from jax import lax
from jax.experimental import pallas as pl
from jax.experimental.pallas import tpu as pltpu
from jax.sharding import PartitionSpec as P

ITERS = 2
MESH = pl.DeviceIdType.MESH
F32 = jnp.float32
BF16 = jnp.bfloat16
B = 256


def split(value):
    high = value.astype(BF16)
    low = (value - high.astype(F32)).astype(BF16)
    return high, low


def dot3(left, right, nt):
    dims = (((1,), (1 if nt else 0,)), ((), ()))

    def one(x, y):
        return lax.dot_general(x, y, dims, preferred_element_type=F32)

    return one(left[0], right[0]) + one(left[0], right[1]) + one(left[1], right[0])


def make_kernel(n_blk, tile):
    own = pl.ds(B, tile)
    other = pl.ds(B + tile, tile)
    row0, row1, row2 = pl.ds(0, B), pl.ds(B, B), pl.ds(2 * B, B)
    rows_of = (row0, row1, row2)
    low_own, low_other = pl.ds(0, tile), pl.ds(tile, tile)
    top_own, top_other = pl.ds(2 * B, tile), pl.ds(2 * B + tile, tile)

    def col(slot, half):
        return pl.ds(slot * B + half * tile, tile)

    def cols(slot):
        return pl.ds(slot * B, B)

    def kernel(s_hbm, h_hbm, zp_hbm, out_ref, sn, z0, z1, d0, d1, so_dn, so_up, sx_dn, kbuf, kx,
               s_hi, s_lo, z_hi, z_lo, d_hi, d_lo, zp_ref, lsem, ssem, rsem):
        side = lax.axis_index("side")
        blk = lax.axis_index("blk")
        partner = {"side": 1 - side}
        up = {"blk": blk + 1}
        dn = {"blk": blk - 1}
        has_up = blk < n_blk - 1
        has_dn = blk > 0

        barrier = pltpu.get_barrier_semaphore()
        pl.semaphore_signal(barrier, inc=1, device_id=partner, device_id_type=MESH)

        @pl.when(has_up)
        def _():
            pl.semaphore_signal(barrier, inc=1, device_id=up, device_id_type=MESH)

        @pl.when(has_dn)
        def _():
            pl.semaphore_signal(barrier, inc=1, device_id=dn, device_id_type=MESH)

        def half_of(g):
            return side if g == 0 else 1 - side

        h_loads = [
            pltpu.make_async_copy(h_hbm.at[:, pl.ds(e * tile, tile)], z0.at[own, col(e, 0)], lsem.at[6 + e])
            for e in range(3)
        ]
        s_loads = []
        for e in range(3):
            for g in range(2):
                src = s_hbm.at[:, pl.ds(pl.multiple_of((2 * e + half_of(g)) * tile, tile), tile)]
                s_loads.append(pltpu.make_async_copy(src, sn.at[own, col(e, g)], lsem.at[2 * e + g]))
        zp_load = pltpu.make_async_copy(zp_hbm, zp_ref, lsem.at[9])
        for load in h_loads + s_loads + [zp_load]:
            load.start()
        for load in h_loads + s_loads:
            load.wait()

        inner = jnp.logical_and(has_up, has_dn)

        @pl.when(inner)
        def _():
            pl.semaphore_wait(barrier, 3)

        @pl.when(jnp.logical_not(inner))
        def _():
            pl.semaphore_wait(barrier, 2)

        used = []

        def remote(src, dst, where):
            i = len(used)
            copy = pltpu.make_async_remote_copy(
                src_ref=src, dst_ref=dst, send_sem=ssem.at[i], recv_sem=rsem.at[i],
                device_id={"x": partner, "u": up, "d": dn}[where], device_id_type=MESH)
            used.append((copy, where))
            return copy

        def start(ups, dns):
            if ups:
                @pl.when(has_up)
                def _():
                    for c in ups:
                        c.start()
            if dns:
                @pl.when(has_dn)
                def _():
                    for c in dns:
                        c.start()

        def receive(ups, dns):
            if ups:
                @pl.when(has_dn)
                def _():
                    for c in ups:
                        c.wait_recv()
            if dns:
                @pl.when(has_up)
                def _():
                    for c in dns:
                        c.wait_recv()

        x_z = [remote(z0.at[own, col(e, 0)], z0.at[other, col(e, 1)], "x") for e in range(3)]
        x_s1 = remote(sn.at[own, col(1, 0)], sn.at[other, col(1, 1)], "x")
        x_s2 = remote(sn.at[own, col(2, 0)], sn.at[other, col(2, 1)], "x")
        x_k = remote(kbuf, kx, "x")
        for c in (x_z[0], x_z[2], x_s1, x_s2, x_z[1]):
            c.start()

        u_own = [
            remote(z0.at[own, col(2, 0)], z0.at[low_own, col(1, 0)], "u"),
            remote(sn.at[own, cols(1)], sn.at[low_own, cols(0)], "u"),
            remote(sn.at[own, col(2, 1)], so_dn, "u"),
            remote(z0.at[own, col(1, 0)], z0.at[low_own, col(0, 0)], "u"),
        ]
        d_own = [
            remote(z0.at[own, col(0, 0)], z0.at[top_own, col(1, 0)], "d"),
            remote(sn.at[own, cols(1)], sn.at[top_own, cols(2)], "d"),
            remote(sn.at[own, col(0, 1)], so_up, "d"),
            remote(z0.at[own, col(1, 0)], z0.at[top_own, col(2, 0)], "d"),
        ]
        start(u_own, d_own)

        zp_load.wait()
        keep_own = [zp_ref[0, 2 * e + half_of(g)].astype(F32) for e in range(3) for g in range(2)]
        row_id = lax.broadcasted_iota(jnp.int32, (8, tile), 0)
        packed = jnp.zeros((8, tile), F32)
        for r in range(6):
            packed = jnp.where(row_id == r, keep_own[r], packed)
        kbuf[...] = packed

        zero = jnp.zeros((tile, tile), F32)
        for e in range(3):
            z0[own, col(e, 1)] = zero
            z0[other, col(e, 0)] = zero
        for e in (0, 1):
            z0[low_own, col(e, 1)] = zero
            z0[low_other, col(e, 0)] = zero
            z0[top_own, col(e + 1, 1)] = zero
            z0[top_other, col(e + 1, 0)] = zero

        @pl.when(jnp.logical_not(has_dn))
        def _():
            for e in (0, 1):
                z0[low_own, col(e, 0)] = zero
                z0[low_other, col(e, 1)] = zero
                for ref in (z1, d0, d1):
                    ref[row0, cols(e)] = jnp.zeros((B, B), F32)
            sn[low_own, cols(0)] = jnp.zeros((tile, B), F32)
            sn[low_other, col(0, 1)] = zero
            so_dn[...] = zero
            sx_dn[...] = zero

        @pl.when(jnp.logical_not(has_up))
        def _():
            for e in (1, 2):
                z0[top_own, col(e, 0)] = zero
                z0[top_other, col(e, 1)] = zero
                for ref in (z1, d0, d1):
                    ref[row2, cols(e)] = jnp.zeros((B, B), F32)
            sn[top_own, cols(2)] = jnp.zeros((tile, B), F32)
            sn[top_other, col(2, 1)] = zero
            so_up[...] = zero

        x_k.start()

        s_refs, z_refs, d_refs = (s_hi, s_lo), (z_hi, z_lo), (d_hi, d_lo)

        def keep_split(refs, row, slot, value):
            high, low = split(value)
            refs[0][rows_of[row], cols(slot)] = high
            refs[1][rows_of[row], cols(slot)] = low

        def load_split(ref, refs, places):
            for row, slot in places:
                keep_split(refs, row, slot, ref[rows_of[row], cols(slot)])

        def pick(refs, rows, columns):
            return refs[0][rows, columns], refs[1][rows, columns]

        def near(refs, row, slot):
            return pick(refs, rows_of[row], cols(slot))

        def nn(left, right):
            return dot3(left, right, False)

        def nt(left, right):
            return dot3(left, right, True)

        sn[other, col(1, 0)] = sn[own, col(1, 1)].T
        x_z[0].wait_recv()
        d_z0 = remote(z0.at[other, col(0, 1)], z0.at[top_other, col(1, 1)], "d")
        start([], [d_z0])
        x_z[2].wait_recv()
        u_z2 = remote(z0.at[other, col(2, 1)], z0.at[low_other, col(1, 1)], "u")
        start([u_z2], [])
        x_s1.wait_recv()
        u_s1 = remote(sn.at[other, col(1, 1)], sn.at[low_other, col(0, 1)], "u")
        d_s1 = remote(sn.at[other, col(1, 1)], sn.at[top_other, col(2, 1)], "d")
        start([u_s1], [d_s1])
        x_s2.wait_recv()
        u_s2 = remote(sn.at[other, col(2, 1)], sx_dn, "u")
        start([u_s2], [])
        x_z[1].wait_recv()
        u_z1 = remote(z0.at[other, col(1, 1)], z0.at[low_other, col(0, 1)], "u")
        d_z1 = remote(z0.at[other, col(1, 1)], z0.at[top_other, col(2, 1)], "d")
        start([u_z1], [d_z1])
        load_split(z0, z_refs, ((1, 0), (1, 1), (1, 2)))
        load_split(sn, s_refs, ((1, 1),))

        receive(u_own, d_own)
        sn[other, col(0, 0)] = so_dn[...].T
        sn[other, col(2, 0)] = so_up[...].T
        sn[low_other, col(0, 0)] = sn[low_own, col(0, 1)].T
        sn[top_other, col(2, 0)] = sn[top_own, col(2, 1)].T
        load_split(sn, s_refs, ((1, 2),))
        receive([u_z2, u_s1], [d_z0, d_s1])
        load_split(sn, s_refs, ((0, 0), (2, 2)))
        receive([u_s2], [])
        sn[other, col(0, 1)] = sx_dn[...].T
        load_split(sn, s_refs, ((1, 0),))
        ups, dns = [u_z1], [d_z1]

        eye = (lax.broadcasted_iota(jnp.int32, (B, B), 0) == lax.broadcasted_iota(jnp.int32, (B, B), 1)).astype(F32)

        for step in range(ITERS):
            last = step == ITERS - 1
            z, d = (z0, d0) if step == 0 else (z1, d1)

            mid = split(z[row1, cols(1)].T)
            t_own = [nn(mid, near(s_refs, 1, 0)), nt(mid, near(s_refs, 1, 1)), nn(mid, near(s_refs, 1, 2))]
            if step > 0:
                receive(*edge)
            load_split(z, z_refs, ((0, 1), (2, 1)))
            lower = split(z[row0, cols(1)].T)
            upper = split(z[row2, cols(1)].T)
            t = [
                split(t_own[0] + nn(lower, near(s_refs, 0, 0))),
                split(t_own[1] + nt(lower, near(s_refs, 1, 0)) + nt(upper, near(s_refs, 1, 2))),
                split(t_own[2] + nn(upper, near(s_refs, 2, 2))),
            ]
            value = eye - (nn(t[0], near(z_refs, 0, 1)) + nn(t[1], near(z_refs, 1, 1)) + nn(t[2], near(z_refs, 2, 1)))
            d[row1, cols(1)] = value
            u_diag = [
                remote(d.at[own, cols(1)], d.at[low_own, cols(0)], "u"),
                remote(d.at[other, col(1, 1)], d.at[low_other, col(0, 1)], "u"),
            ]
            d_diag = [
                remote(d.at[own, cols(1)], d.at[top_own, cols(2)], "d"),
                remote(d.at[other, col(1, 1)], d.at[top_other, col(2, 1)], "d"),
            ]
            start(u_diag, d_diag)
            keep_split(d_refs, 1, 1, value)

            receive(ups, dns)
            load_split(z, z_refs, ((0, 0), (2, 2)))
            value = -(nn(t[1], near(z_refs, 1, 2)) + nn(t[2], near(z_refs, 2, 2)))
            d[row1, cols(2)] = value
            u_edge = remote(d.at[row1, cols(2)], d.at[row0, cols(1)], "u")
            start([u_edge], [])
            keep_split(d_refs, 1, 2, value)
            value = -(nn(t[0], near(z_refs, 0, 0)) + nn(t[1], near(z_refs, 1, 0)))
            d[row1, cols(0)] = value
            d_edge = remote(d.at[row1, cols(0)], d.at[row2, cols(1)], "d")
            start([], [d_edge])
            keep_split(d_refs, 1, 0, value)

            mine = own if last else row1
            left = [pick(z_refs, mine, cols(k)) for k in range(3)]
            first = [None, None, None]
            first[1] = sum(nt(left[k], near(d_refs, 1, k)) for k in range(3))
            f_mid = split(first[1])
            second_mid = nt(f_mid, near(d_refs, 1, 1))
            receive(u_diag, d_diag)
            d[low_other, col(0, 0)] = d[low_own, col(0, 1)].T
            d[top_other, col(2, 0)] = d[top_own, col(2, 1)].T
            load_split(d, d_refs, ((0, 0), (2, 2)))
            first[0] = nt(left[0], near(d_refs, 0, 0))
            first[2] = nt(left[2], near(d_refs, 2, 2))
            if step == 0:
                x_k.wait_recv()

            def finish(slot, second):
                value = z[mine, cols(slot)] + 0.5 * first[slot] + 0.375 * second
                for g in range(2):
                    part = value[:tile, g * tile:(g + 1) * tile]
                    if not (slot == 1 and g == 0):
                        part = part * keep_own[2 * slot + g]
                    if last:
                        out_ref[:, pl.ds(pl.multiple_of((2 * slot + half_of(g)) * tile, tile), tile)] = part
                        continue
                    z1[own, col(slot, g)] = part
                    part = value[tile:, g * tile:(g + 1) * tile]
                    if not (slot == 1 and g == 1):
                        r = 2 * slot + 1 - g
                        part = part * kx[r:r + 1, :]
                    z1[other, col(slot, g)] = part

            receive([u_edge], [])
            load_split(d, d_refs, ((0, 1),))
            first[0] = first[0] + nt(left[1], near(d_refs, 0, 1))
            f_low = split(first[0])
            finish(0, nt(f_low, near(d_refs, 0, 0)) + nt(f_mid, near(d_refs, 0, 1)))
            edge = [[], []]
            if not last:
                edge[1].append(remote(z1.at[row1, cols(0)], z1.at[row2, cols(1)], "d"))
                start([], edge[1])
            receive([], [d_edge])
            load_split(d, d_refs, ((2, 1),))
            first[2] = first[2] + nt(left[1], near(d_refs, 2, 1))
            f_high = split(first[2])
            finish(2, nt(f_mid, near(d_refs, 2, 1)) + nt(f_high, near(d_refs, 2, 2)))
            if not last:
                edge[0].append(remote(z1.at[row1, cols(2)], z1.at[row0, cols(1)], "u"))
                start(edge[0], [])
            finish(1, second_mid + nt(f_low, near(d_refs, 1, 0)) + nt(f_high, near(d_refs, 1, 2)))
            if not last:
                ups = [remote(z1.at[row1, cols(1)], z1.at[row0, cols(0)], "u")]
                dns = [remote(z1.at[row1, cols(1)], z1.at[row2, cols(2)], "d")]
                start(ups, dns)
                load_split(z1, z_refs, ((1, 0), (1, 1), (1, 2)))

        for c, where in used:
            if where == "x":
                c.wait_send()

        @pl.when(has_up)
        def _():
            for c, where in used:
                if where == "u":
                    c.wait_send()

        @pl.when(has_dn)
        def _():
            for c, where in used:
                if where == "d":
                    c.wait_send()

    return kernel


def solution(mesh):
    n_blk = mesh.shape["blk"]

    def per_device(intersect, half_factors, z_pattern):
        tile = intersect.shape[0]
        near = pltpu.VMEM((3 * B, 3 * B), F32)
        half = pltpu.VMEM((3 * B, 3 * B), BF16)
        block = pltpu.VMEM((tile, tile), F32)
        return pl.pallas_call(
            make_kernel(n_blk, tile),
            out_shape=jax.ShapeDtypeStruct(intersect.shape, F32),
            in_specs=[
                pl.BlockSpec(memory_space=pltpu.HBM),
                pl.BlockSpec(memory_space=pltpu.HBM),
                pl.BlockSpec(memory_space=pltpu.HBM),
            ],
            out_specs=pl.BlockSpec(memory_space=pltpu.VMEM),
            scratch_shapes=[near] * 5 + [block] * 3 + [pltpu.VMEM((8, tile), F32)] * 2 + [half] * 6

            + [pltpu.SMEM((1, 6), jnp.int32), pltpu.SemaphoreType.DMA((10,)), pltpu.SemaphoreType.DMA((48,)), pltpu.SemaphoreType.DMA((48,))],
            compiler_params=pltpu.CompilerParams(
                collective_id=0, has_side_effects=True, vmem_limit_bytes=48 * 1024 * 1024),
            name="merge",
        )(intersect, half_factors, z_pattern)

    spec = P(("pair", "side", "blk"), None)
    return jax.shard_map(per_device, mesh=mesh, in_specs=(spec,) * 3, out_specs=spec, check_vma=False)
```

```python
import jax
import jax.numpy as jnp
from jax import lax
from jax.experimental import pallas as pl
from jax.experimental.pallas import tpu as pltpu
from jax.sharding import PartitionSpec as P

ITERS = 2
MESH = pl.DeviceIdType.MESH
F32 = jnp.float32
BF16 = jnp.bfloat16
B = 256


def split(value):
    high = value.astype(BF16)
    low = (value - high.astype(F32)).astype(BF16)
    return high, low


def lanes(shape):
    return lax.broadcasted_iota(jnp.int32, shape, 1)


def store_packed(ref, start, tile):
    ref[pl.ds(start, 32), :] = tile[0:32]
    ref[pl.ds(start + 32, 32), :] = jnp.where(lanes((32, 128)) < 32, pltpu.roll(tile[96:128], 32, 1), tile[32:64])
    ref[pl.ds(start + 64, 16), :] = jnp.where(lanes((16, 128)) < 64, pltpu.roll(tile[80:96], 64, 1), tile[64:80])


def load_packed(ref, start):
    first = ref[pl.ds(start, 32), :]
    second = ref[pl.ds(start + 32, 32), :]
    third = ref[pl.ds(start + 64, 16), :]
    upper = jnp.concatenate(
        [first, second, third, pltpu.roll(third, 64, 1), pltpu.roll(second, 96, 1)], axis=0)
    row = lax.broadcasted_iota(jnp.int32, (128, 128), 0)
    return jnp.where(lanes((128, 128)) >= row, upper, upper.T)


def dot3(left, right, nt):
    dims = (((1,), (1 if nt else 0,)), ((), ()))

    def one(x, y):
        return lax.dot_general(x, y, dims, preferred_element_type=F32)

    return one(left[0], right[0]) + one(left[0], right[1]) + one(left[1], right[0])


def make_kernel(n_blk, tile):
    own = pl.ds(B, tile)
    other = pl.ds(B + tile, tile)
    row0, row1, row2 = pl.ds(0, B), pl.ds(B, B), pl.ds(2 * B, B)
    rows_of = (row0, row1, row2)
    low_own, low_other = pl.ds(0, tile), pl.ds(tile, tile)
    top_own, top_other = pl.ds(2 * B, tile), pl.ds(2 * B + tile, tile)

    def col(slot, half):
        return pl.ds(slot * B + half * tile, tile)

    def cols(slot):
        return pl.ds(slot * B, B)

    def kernel(s_hbm, h_hbm, zp_hbm, out_ref, sn, z0, z1, d0, d1, so_dn, so_up, sx_dn, sp, sx, spo_dn, spo_up, spx_dn, spx_up,
               pd0, pd1, qdn0, qdn1, qup0, qup1, kbuf, kx,
               s_hi, s_lo, z_hi, z_lo, d_hi, d_lo, zp_ref, lsem, ssem, rsem):
        side = lax.axis_index("side")
        blk = lax.axis_index("blk")
        partner = {"side": 1 - side}
        up = {"blk": blk + 1}
        dn = {"blk": blk - 1}
        has_up = blk < n_blk - 1
        has_dn = blk > 0

        barrier = pltpu.get_barrier_semaphore()
        pl.semaphore_signal(barrier, inc=1, device_id=partner, device_id_type=MESH)

        @pl.when(has_up)
        def _():
            pl.semaphore_signal(barrier, inc=1, device_id=up, device_id_type=MESH)

        @pl.when(has_dn)
        def _():
            pl.semaphore_signal(barrier, inc=1, device_id=dn, device_id_type=MESH)

        def half_of(g):
            return side if g == 0 else 1 - side

        h_loads = [
            pltpu.make_async_copy(h_hbm.at[:, pl.ds(e * tile, tile)], z0.at[own, col(e, 0)], lsem.at[6 + e])
            for e in range(3)
        ]
        s_loads = []
        for e in range(3):
            for g in range(2):
                src = s_hbm.at[:, pl.ds(pl.multiple_of((2 * e + half_of(g)) * tile, tile), tile)]
                s_loads.append(pltpu.make_async_copy(src, sn.at[own, col(e, g)], lsem.at[2 * e + g]))
        zp_load = pltpu.make_async_copy(zp_hbm, zp_ref, lsem.at[9])
        for load in h_loads + s_loads + [zp_load]:
            load.start()
        for load in h_loads + s_loads:
            load.wait()

        inner = jnp.logical_and(has_up, has_dn)

        @pl.when(inner)
        def _():
            pl.semaphore_wait(barrier, 3)

        @pl.when(jnp.logical_not(inner))
        def _():
            pl.semaphore_wait(barrier, 2)

        used = []

        def remote(src, dst, where):
            i = len(used)
            copy = pltpu.make_async_remote_copy(
                src_ref=src, dst_ref=dst, send_sem=ssem.at[i], recv_sem=rsem.at[i],
                device_id={"x": partner, "u": up, "d": dn}[where], device_id_type=MESH)
            used.append((copy, where))
            return copy

        def start(ups, dns):
            if ups:
                @pl.when(has_up)
                def _():
                    for c in ups:
                        c.start()
            if dns:
                @pl.when(has_dn)
                def _():
                    for c in dns:
                        c.start()

        def receive(ups, dns):
            if ups:
                @pl.when(has_dn)
                def _():
                    for c in ups:
                        c.wait_recv()
            if dns:
                @pl.when(has_up)
                def _():
                    for c in dns:
                        c.wait_recv()

        x_z = [remote(z0.at[own, col(e, 0)], z0.at[other, col(e, 1)], "x") for e in range(3)]
        x_s1 = remote(sp, sx, "x")
        x_s2 = remote(sn.at[own, col(2, 0)], sn.at[other, col(2, 1)], "x")
        x_k = remote(kbuf, kx, "x")
        for c in (x_z[0], x_z[2], x_s2):
            c.start()
        store_packed(sp, 0, sn[own, col(1, 0)])
        x_s1.start()
        x_z[1].start()

        u_own = [
            remote(z0.at[own, col(2, 0)], z0.at[low_own, col(1, 0)], "u"),
            remote(sp, spo_dn, "u"),
            remote(sn.at[own, col(1, 1)], sn.at[low_own, col(0, 1)], "u"),
            remote(sn.at[own, col(2, 1)], so_dn, "u"),
            remote(z0.at[own, col(1, 0)], z0.at[low_own, col(0, 0)], "u"),
        ]
        d_own = [
            remote(z0.at[own, col(0, 0)], z0.at[top_own, col(1, 0)], "d"),
            remote(sp, spo_up, "d"),
            remote(sn.at[own, col(1, 1)], sn.at[top_own, col(2, 1)], "d"),
            remote(sn.at[own, col(0, 1)], so_up, "d"),
            remote(z0.at[own, col(1, 0)], z0.at[top_own, col(2, 0)], "d"),
        ]
        start(u_own, d_own)

        zp_load.wait()
        keep_own = [zp_ref[0, 2 * e + half_of(g)].astype(F32) for e in range(3) for g in range(2)]
        row_id = lax.broadcasted_iota(jnp.int32, (8, tile), 0)
        packed = jnp.zeros((8, tile), F32)
        for r in range(6):
            packed = jnp.where(row_id == r, keep_own[r], packed)
        kbuf[...] = packed

        zero = jnp.zeros((tile, tile), F32)
        for e in range(3):
            z0[own, col(e, 1)] = zero
            z0[other, col(e, 0)] = zero
        for e in (0, 1):
            z0[low_own, col(e, 1)] = zero
            z0[low_other, col(e, 0)] = zero
            z0[top_own, col(e + 1, 1)] = zero
            z0[top_other, col(e + 1, 0)] = zero

        @pl.when(jnp.logical_not(has_dn))
        def _():
            for e in (0, 1):
                z0[low_own, col(e, 0)] = zero
                z0[low_other, col(e, 1)] = zero
                z1[row0, cols(e)] = jnp.zeros((B, B), F32)
            for ref in (d0, d1):
                ref[row0, cols(1)] = jnp.zeros((B, B), F32)
            for ref in (spo_dn, spx_dn, qdn0, qdn1):
                ref[...] = jnp.zeros(ref.shape, F32)
            sn[low_own, col(0, 1)] = zero
            so_dn[...] = zero
            sx_dn[...] = zero

        @pl.when(jnp.logical_not(has_up))
        def _():
            for e in (1, 2):
                z0[top_own, col(e, 0)] = zero
                z0[top_other, col(e, 1)] = zero
                z1[row2, cols(e)] = jnp.zeros((B, B), F32)
            for ref in (d0, d1):
                ref[row2, cols(1)] = jnp.zeros((B, B), F32)
            for ref in (spo_up, spx_up, qup0, qup1):
                ref[...] = jnp.zeros(ref.shape, F32)
            sn[top_own, col(2, 1)] = zero
            so_up[...] = zero

        x_k.start()

        s_refs, z_refs, d_refs = (s_hi, s_lo), (z_hi, z_lo), (d_hi, d_lo)

        def keep_split(refs, row, slot, value):
            high, low = split(value)
            refs[0][rows_of[row], cols(slot)] = high
            refs[1][rows_of[row], cols(slot)] = low

        def load_split(ref, refs, places):
            for row, slot in places:
                keep_split(refs, row, slot, ref[rows_of[row], cols(slot)])

        def pick(refs, rows, columns):
            return refs[0][rows, columns], refs[1][rows, columns]

        def near(refs, row, slot):
            return pick(refs, rows_of[row], cols(slot))

        def nn(left, right):
            return dot3(left, right, False)

        def nt(left, right):
            return dot3(left, right, True)

        sn[other, col(1, 0)] = sn[own, col(1, 1)].T
        x_z[0].wait_recv()
        d_z0 = remote(z0.at[other, col(0, 1)], z0.at[top_other, col(1, 1)], "d")
        start([], [d_z0])
        x_z[2].wait_recv()
        u_z2 = remote(z0.at[other, col(2, 1)], z0.at[low_other, col(1, 1)], "u")
        start([u_z2], [])
        x_s2.wait_recv()
        u_s2 = remote(sn.at[other, col(2, 1)], sx_dn, "u")
        start([u_s2], [])
        x_s1.wait_recv()
        u_s1 = remote(sx, spx_dn, "u")
        d_s1 = remote(sx, spx_up, "d")
        start([u_s1], [d_s1])
        sn[other, col(1, 1)] = load_packed(sx, 0)
        load_split(sn, s_refs, ((1, 1),))

        receive(u_own, d_own)
        sn[other, col(0, 0)] = so_dn[...].T
        sn[other, col(2, 0)] = so_up[...].T
        sn[low_own, col(0, 0)] = load_packed(spo_dn, 0)
        sn[top_own, col(2, 0)] = load_packed(spo_up, 0)
        sn[low_other, col(0, 0)] = sn[low_own, col(0, 1)].T
        sn[top_other, col(2, 0)] = sn[top_own, col(2, 1)].T
        load_split(sn, s_refs, ((1, 2),))
        receive([u_z2], [d_z0])
        load_split(z0, z_refs, ((0, 1), (2, 1), (1, 0), (1, 2)))
        lower = split(z0[row0, cols(1)].T)
        upper = split(z0[row2, cols(1)].T)

        x_z[1].wait_recv()
        u_z1 = remote(z0.at[other, col(1, 1)], z0.at[low_other, col(0, 1)], "u")
        d_z1 = remote(z0.at[other, col(1, 1)], z0.at[top_other, col(2, 1)], "d")
        start([u_z1], [d_z1])
        load_split(z0, z_refs, ((1, 1),))
        receive([u_s2, u_s1], [d_s1])
        sn[other, col(0, 1)] = sx_dn[...].T
        load_split(sn, s_refs, ((1, 0),))
        sn[low_other, col(0, 1)] = load_packed(spx_dn, 0)
        sn[top_other, col(2, 1)] = load_packed(spx_up, 0)
        load_split(sn, s_refs, ((0, 0), (2, 2)))
        ups, dns = [u_z1], [d_z1]

        eye = (lax.broadcasted_iota(jnp.int32, (B, B), 0) == lax.broadcasted_iota(jnp.int32, (B, B), 1)).astype(F32)

        for step in range(ITERS):
            last = step == ITERS - 1
            z, d = (z0, d0) if step == 0 else (z1, d1)
            pd, q_dn, q_up = (pd0, qdn0, qup0) if step == 0 else (pd1, qdn1, qup1)

            mid = split(z[row1, cols(1)].T)
            t_own = [nn(mid, near(s_refs, 1, 0)), nt(mid, near(s_refs, 1, 1)), nn(mid, near(s_refs, 1, 2))]
            if step > 0:
                receive(*edge)
                load_split(z, z_refs, ((0, 1), (2, 1)))
                lower = split(z[row0, cols(1)].T)
                upper = split(z[row2, cols(1)].T)
            t = [
                split(t_own[0] + nn(lower, near(s_refs, 0, 0))),
                split(t_own[1] + nt(lower, near(s_refs, 1, 0)) + nt(upper, near(s_refs, 1, 2))),
                split(t_own[2] + nn(upper, near(s_refs, 2, 2))),
            ]
            value = eye - (nn(t[0], near(z_refs, 0, 1)) + nn(t[1], near(z_refs, 1, 1)) + nn(t[2], near(z_refs, 2, 1)))
            store_packed(pd, 0, value[:tile, :tile])
            pd[pl.ds(80, tile), :] = value[:tile, tile:]
            store_packed(pd, 80 + tile, value[tile:, tile:])
            u_diag, d_diag = [remote(pd, q_dn, "u")], [remote(pd, q_up, "d")]
            start(u_diag, d_diag)
            keep_split(d_refs, 1, 1, value)

            receive(ups, dns)
            load_split(z, z_refs, ((0, 0), (2, 2)))
            value = -(nn(t[1], near(z_refs, 1, 2)) + nn(t[2], near(z_refs, 2, 2)))
            d[row1, cols(2)] = value
            u_edge = remote(d.at[row1, cols(2)], d.at[row0, cols(1)], "u")
            start([u_edge], [])
            keep_split(d_refs, 1, 2, value)
            value = -(nn(t[0], near(z_refs, 0, 0)) + nn(t[1], near(z_refs, 1, 0)))
            d[row1, cols(0)] = value
            d_edge = remote(d.at[row1, cols(0)], d.at[row2, cols(1)], "d")
            start([], [d_edge])
            keep_split(d_refs, 1, 0, value)

            mine = own if last else row1
            left = [pick(z_refs, mine, cols(k)) for k in range(3)]
            first = [None, None, None]
            first[1] = sum(nt(left[k], near(d_refs, 1, k)) for k in range(3))
            f_mid = split(first[1])
            second_mid = nt(f_mid, near(d_refs, 1, 1))
            receive(u_diag, d_diag)
            for row, ref in ((0, q_dn), (2, q_up)):
                cross = ref[pl.ds(80, tile), :]
                top = jnp.concatenate([load_packed(ref, 0), cross], axis=1)
                low = jnp.concatenate([cross.T, load_packed(ref, 80 + tile)], axis=1)
                keep_split(d_refs, row, row, jnp.concatenate([top, low], axis=0))
            first[0] = nt(left[0], near(d_refs, 0, 0))
            first[2] = nt(left[2], near(d_refs, 2, 2))
            if step == 0:
                x_k.wait_recv()

            def finish(slot, second):
                value = z[mine, cols(slot)] + 0.5 * first[slot] + 0.375 * second
                for g in range(2):
                    part = value[:tile, g * tile:(g + 1) * tile]
                    if not (slot == 1 and g == 0):
                        part = part * keep_own[2 * slot + g]
                    if last:
                        out_ref[:, pl.ds(pl.multiple_of((2 * slot + half_of(g)) * tile, tile), tile)] = part
                        continue
                    z1[own, col(slot, g)] = part
                    part = value[tile:, g * tile:(g + 1) * tile]
                    if not (slot == 1 and g == 1):
                        r = 2 * slot + 1 - g
                        part = part * kx[r:r + 1, :]
                    z1[other, col(slot, g)] = part

            receive([u_edge], [])
            load_split(d, d_refs, ((0, 1),))
            first[0] = first[0] + nt(left[1], near(d_refs, 0, 1))
            f_low = split(first[0])
            finish(0, nt(f_low, near(d_refs, 0, 0)) + nt(f_mid, near(d_refs, 0, 1)))
            edge = [[], []]
            if not last:
                edge[1].append(remote(z1.at[row1, cols(0)], z1.at[row2, cols(1)], "d"))
                start([], edge[1])
            receive([], [d_edge])
            load_split(d, d_refs, ((2, 1),))
            first[2] = first[2] + nt(left[1], near(d_refs, 2, 1))
            f_high = split(first[2])
            finish(2, nt(f_mid, near(d_refs, 2, 1)) + nt(f_high, near(d_refs, 2, 2)))
            if not last:
                edge[0].append(remote(z1.at[row1, cols(2)], z1.at[row0, cols(1)], "u"))
                start(edge[0], [])
            finish(1, second_mid + nt(f_low, near(d_refs, 1, 0)) + nt(f_high, near(d_refs, 1, 2)))
            if not last:
                ups = [remote(z1.at[row1, cols(1)], z1.at[row0, cols(0)], "u")]
                dns = [remote(z1.at[row1, cols(1)], z1.at[row2, cols(2)], "d")]
                start(ups, dns)
                load_split(z1, z_refs, ((1, 0), (1, 1), (1, 2)))

        for c, where in used:
            if where == "x":
                c.wait_send()

        @pl.when(has_up)
        def _():
            for c, where in used:
                if where == "u":
                    c.wait_send()

        @pl.when(has_dn)
        def _():
            for c, where in used:
                if where == "d":
                    c.wait_send()

    return kernel


def solution(mesh):
    n_blk = mesh.shape["blk"]

    def per_device(intersect, half_factors, z_pattern):
        tile = intersect.shape[0]
        near = pltpu.VMEM((3 * B, 3 * B), F32)
        half = pltpu.VMEM((3 * B, 3 * B), BF16)
        block = pltpu.VMEM((tile, tile), F32)
        packed = pltpu.VMEM((80, tile), F32)
        message = pltpu.VMEM((160 + tile, tile), F32)
        return pl.pallas_call(
            make_kernel(n_blk, tile),
            out_shape=jax.ShapeDtypeStruct(intersect.shape, F32),
            in_specs=[
                pl.BlockSpec(memory_space=pltpu.HBM),
                pl.BlockSpec(memory_space=pltpu.HBM),
                pl.BlockSpec(memory_space=pltpu.HBM),
            ],
            out_specs=pl.BlockSpec(memory_space=pltpu.VMEM),
            scratch_shapes=[near] * 5 + [block] * 3 + [packed] * 6 + [message] * 6 + [pltpu.VMEM((8, tile), F32)] * 2 + [half] * 6

            + [pltpu.SMEM((1, 6), jnp.int32), pltpu.SemaphoreType.DMA((10,)), pltpu.SemaphoreType.DMA((48,)), pltpu.SemaphoreType.DMA((48,))],
            compiler_params=pltpu.CompilerParams(
                collective_id=0, has_side_effects=True, vmem_limit_bytes=48 * 1024 * 1024),
            name="merge",
        )(intersect, half_factors, z_pattern)

    spec = P(("pair", "side", "blk"), None)
    return jax.shard_map(per_device, mesh=mesh, in_specs=(spec,) * 3, out_specs=spec, check_vma=False)
```

```python
import jax
import jax.numpy as jnp
from jax import lax
from jax.experimental import pallas as pl
from jax.experimental.pallas import tpu as pltpu
from jax.sharding import PartitionSpec as P

ITERS = 2
MESH = pl.DeviceIdType.MESH
F32 = jnp.float32
BF16 = jnp.bfloat16
B = 256


def split(value):
    high = value.astype(BF16)
    low = (value - high.astype(F32)).astype(BF16)
    return high, low


def lanes(shape):
    return lax.broadcasted_iota(jnp.int32, shape, 1)


def store_packed(ref, start, tile):
    ref[pl.ds(start, 32), :] = tile[0:32]
    ref[pl.ds(start + 32, 32), :] = jnp.where(lanes((32, 128)) < 32, pltpu.roll(tile[96:128], 32, 1), tile[32:64])
    ref[pl.ds(start + 64, 16), :] = jnp.where(lanes((16, 128)) < 64, pltpu.roll(tile[80:96], 64, 1), tile[64:80])


def load_packed(ref, start):
    first = ref[pl.ds(start, 32), :]
    second = ref[pl.ds(start + 32, 32), :]
    third = ref[pl.ds(start + 64, 16), :]
    upper = jnp.concatenate(
        [first, second, third, pltpu.roll(third, 64, 1), pltpu.roll(second, 96, 1)], axis=0)
    row = lax.broadcasted_iota(jnp.int32, (128, 128), 0)
    return jnp.where(lanes((128, 128)) >= row, upper, upper.T)


def dot3(left, right, nt):
    dims = (((1,), (1 if nt else 0,)), ((), ()))

    def one(x, y):
        return lax.dot_general(x, y, dims, preferred_element_type=F32)

    return one(left[0], right[0]) + one(left[0], right[1]) + one(left[1], right[0])


def make_kernel(n_blk, tile):
    own = pl.ds(B, tile)
    other = pl.ds(B + tile, tile)
    row0, row1, row2 = pl.ds(0, B), pl.ds(B, B), pl.ds(2 * B, B)
    rows_of = (row0, row1, row2)
    low_own, low_other = pl.ds(0, tile), pl.ds(tile, tile)
    top_own, top_other = pl.ds(2 * B, tile), pl.ds(2 * B + tile, tile)

    def col(slot, half):
        return pl.ds(slot * B + half * tile, tile)

    def cols(slot):
        return pl.ds(slot * B, B)

    def kernel(s_hbm, h_hbm, zp_hbm, out_ref, sn, z0, z1, d0, d1, so_dn, so_up, sx_dn, sp, sx, spo_dn, spo_up, spx_dn, spx_up,
               pd0, pd1, qdn0, qdn1, qup0, qup1, kbuf, kx,
               s_hi, s_lo, z_hi, z_lo, d_hi, d_lo, zp_ref, lsem, ssem, rsem):
        side = lax.axis_index("side")
        blk = lax.axis_index("blk")
        partner = {"side": 1 - side}
        up = {"blk": blk + 1}
        dn = {"blk": blk - 1}
        has_up = blk < n_blk - 1
        has_dn = blk > 0

        barrier = pltpu.get_barrier_semaphore()
        pl.semaphore_signal(barrier, inc=1, device_id=partner, device_id_type=MESH)

        @pl.when(has_up)
        def _():
            pl.semaphore_signal(barrier, inc=1, device_id=up, device_id_type=MESH)

        @pl.when(has_dn)
        def _():
            pl.semaphore_signal(barrier, inc=1, device_id=dn, device_id_type=MESH)

        def half_of(g):
            return side if g == 0 else 1 - side

        h_loads = [
            pltpu.make_async_copy(h_hbm.at[:, pl.ds(e * tile, tile)], z0.at[own, col(e, 0)], lsem.at[6 + e])
            for e in range(3)
        ]
        s_loads = []
        for e in range(3):
            for g in range(2):
                src = s_hbm.at[:, pl.ds(pl.multiple_of((2 * e + half_of(g)) * tile, tile), tile)]
                s_loads.append(pltpu.make_async_copy(src, sn.at[own, col(e, g)], lsem.at[2 * e + g]))
        zp_load = pltpu.make_async_copy(zp_hbm, zp_ref, lsem.at[9])
        for load in h_loads + s_loads + [zp_load]:
            load.start()
        for load in h_loads + s_loads:
            load.wait()

        inner = jnp.logical_and(has_up, has_dn)

        @pl.when(inner)
        def _():
            pl.semaphore_wait(barrier, 3)

        @pl.when(jnp.logical_not(inner))
        def _():
            pl.semaphore_wait(barrier, 2)

        used = []

        def remote(src, dst, where):
            i = len(used)
            copy = pltpu.make_async_remote_copy(
                src_ref=src, dst_ref=dst, send_sem=ssem.at[i], recv_sem=rsem.at[i],
                device_id={"x": partner, "u": up, "d": dn}[where], device_id_type=MESH)
            used.append((copy, where))
            return copy

        def start(ups, dns):
            if ups:
                @pl.when(has_up)
                def _():
                    for c in ups:
                        c.start()
            if dns:
                @pl.when(has_dn)
                def _():
                    for c in dns:
                        c.start()

        def receive(ups, dns):
            if ups:
                @pl.when(has_dn)
                def _():
                    for c in ups:
                        c.wait_recv()
            if dns:
                @pl.when(has_up)
                def _():
                    for c in dns:
                        c.wait_recv()

        x_z = [remote(z0.at[own, col(e, 0)], z0.at[other, col(e, 1)], "x") for e in range(3)]
        x_s1 = remote(sp, sx, "x")
        x_s2 = remote(sn.at[own, col(2, 0)], sn.at[other, col(2, 1)], "x")
        x_k = remote(kbuf, kx, "x")
        for c in (x_z[0], x_z[2], x_s2):
            c.start()
        store_packed(sp, 0, sn[own, col(1, 0)])
        x_s1.start()
        x_z[1].start()

        u_own = [
            remote(z0.at[own, col(2, 0)], z0.at[low_own, col(1, 0)], "u"),
            remote(sp, spo_dn, "u"),
            remote(sn.at[own, col(1, 1)], sn.at[low_own, col(0, 1)], "u"),
            remote(sn.at[own, col(2, 1)], so_dn, "u"),
            remote(z0.at[own, col(1, 0)], z0.at[low_own, col(0, 0)], "u"),
        ]
        d_own = [
            remote(z0.at[own, col(0, 0)], z0.at[top_own, col(1, 0)], "d"),
            remote(sp, spo_up, "d"),
            remote(sn.at[own, col(1, 1)], sn.at[top_own, col(2, 1)], "d"),
            remote(sn.at[own, col(0, 1)], so_up, "d"),
            remote(z0.at[own, col(1, 0)], z0.at[top_own, col(2, 0)], "d"),
        ]
        start(u_own, d_own)

        zp_load.wait()
        keep_own = [zp_ref[0, 2 * e + half_of(g)].astype(F32) for e in range(3) for g in range(2)]
        row_id = lax.broadcasted_iota(jnp.int32, (8, tile), 0)
        packed = jnp.zeros((8, tile), F32)
        for r in range(6):
            packed = jnp.where(row_id == r, keep_own[r], packed)
        kbuf[...] = packed

        zero = jnp.zeros((tile, tile), F32)
        for e in range(3):
            z0[own, col(e, 1)] = zero
            z0[other, col(e, 0)] = zero
        for e in (0, 1):
            z0[low_own, col(e, 1)] = zero
            z0[low_other, col(e, 0)] = zero
            z0[top_own, col(e + 1, 1)] = zero
            z0[top_other, col(e + 1, 0)] = zero

        @pl.when(jnp.logical_not(has_dn))
        def _():
            for e in (0, 1):
                z0[low_own, col(e, 0)] = zero
                z0[low_other, col(e, 1)] = zero
                z1[row0, cols(e)] = jnp.zeros((B, B), F32)
            for ref in (d0, d1):
                ref[row0, cols(1)] = jnp.zeros((B, B), F32)
            for ref in (spo_dn, spx_dn, qdn0, qdn1):
                ref[...] = jnp.zeros(ref.shape, F32)
            sn[low_own, col(0, 1)] = zero
            so_dn[...] = zero
            sx_dn[...] = zero

        @pl.when(jnp.logical_not(has_up))
        def _():
            for e in (1, 2):
                z0[top_own, col(e, 0)] = zero
                z0[top_other, col(e, 1)] = zero
                z1[row2, cols(e)] = jnp.zeros((B, B), F32)
            for ref in (d0, d1):
                ref[row2, cols(1)] = jnp.zeros((B, B), F32)
            for ref in (spo_up, spx_up, qup0, qup1):
                ref[...] = jnp.zeros(ref.shape, F32)
            sn[top_own, col(2, 1)] = zero
            so_up[...] = zero

        x_k.start()

        s_refs, z_refs, d_refs = (s_hi, s_lo), (z_hi, z_lo), (d_hi, d_lo)

        def keep_split(refs, row, slot, value):
            high, low = split(value)
            refs[0][rows_of[row], cols(slot)] = high
            refs[1][rows_of[row], cols(slot)] = low

        def load_split(ref, refs, places):
            for row, slot in places:
                keep_split(refs, row, slot, ref[rows_of[row], cols(slot)])

        def pick(refs, rows, columns):
            return refs[0][rows, columns], refs[1][rows, columns]

        def near(refs, row, slot):
            return pick(refs, rows_of[row], cols(slot))

        def nn(left, right):
            return dot3(left, right, False)

        def nt(left, right):
            return dot3(left, right, True)

        low_rows, mid_rows, top_rows = (low_own, low_other), (own, other), (top_own, top_other)

        def load(ref, refs, *places):
            for rows, columns in places:
                high, low = split(ref[rows, columns])
                refs[0][rows, columns] = high
                refs[1][rows, columns] = low

        def put(refs, rows, columns, value):
            high, low = split(value)
            refs[0][rows, columns] = high
            refs[1][rows, columns] = low

        def eye(n):
            return (lax.broadcasted_iota(jnp.int32, (n, n), 0) == lax.broadcasted_iota(jnp.int32, (n, n), 1)).astype(F32)

        def image_rows(h):
            mid = split(z0[mid_rows[h], col(1, h)].T)
            lower = split(z0[low_rows[h], col(1, h)].T)
            upper = split(z0[top_rows[h], col(1, h)].T)
            here = [pick(s_refs, mid_rows[h], cols(k)) for k in range(3)]
            return [
                split(nn(lower, pick(s_refs, low_rows[h], cols(0))) + nn(mid, here[0])),
                split(nt(lower, pick(s_refs, row1, col(0, h))) + nn(mid, here[1]) + nt(upper, pick(s_refs, row1, col(2, h)))),
                split(nn(mid, here[2]) + nn(upper, pick(s_refs, top_rows[h], cols(2)))),
            ]

        def half_cols(pair, h):
            return pair[0][:, h * tile:(h + 1) * tile], pair[1][:, h * tile:(h + 1) * tile]

        def diag_tiles(image, h, slot):
            near_rows = (low_rows[h], mid_rows[h], top_rows[h])
            return sum(nn(half_cols(image[f], h), pick(z_refs, near_rows[f], col(slot, h)))
                       for f in range(3) if abs(f - slot) < 2)

        sn[other, col(1, 0)] = sn[own, col(1, 1)].T
        load(sn, s_refs, (own, cols(0)), (own, cols(1)), (own, cols(2)), (other, col(1, 0)))
        load(z0, z_refs, *[(own, cols(e)) for e in range(3)], *[(other, col(e, 0)) for e in range(3)])
        x_z[0].wait_recv()
        d_z0 = remote(z0.at[other, col(0, 1)], z0.at[top_other, col(1, 1)], "d")
        start([], [d_z0])
        x_z[2].wait_recv()
        u_z2 = remote(z0.at[other, col(2, 1)], z0.at[low_other, col(1, 1)], "u")
        start([u_z2], [])
        x_s2.wait_recv()
        u_s2 = remote(sn.at[other, col(2, 1)], sx_dn, "u")
        start([u_s2], [])
        x_s1.wait_recv()
        u_s1 = remote(sx, spx_dn, "u")
        d_s1 = remote(sx, spx_up, "d")
        start([u_s1], [d_s1])

        receive(u_own, d_own)
        sn[other, col(0, 0)] = so_dn[...].T
        sn[other, col(2, 0)] = so_up[...].T
        sn[low_own, col(0, 0)] = load_packed(spo_dn, 0)
        sn[top_own, col(2, 0)] = load_packed(spo_up, 0)
        sn[low_other, col(0, 0)] = sn[low_own, col(0, 1)].T
        sn[top_other, col(2, 0)] = sn[top_own, col(2, 1)].T
        load(sn, s_refs, (low_own, cols(0)), (top_own, cols(2)), (other, col(0, 0)), (other, col(2, 0)),
             (low_other, col(0, 0)), (top_other, col(2, 0)))
        load(z0, z_refs, (low_own, cols(0)), (low_own, cols(1)), (top_own, cols(1)), (top_own, cols(2)),
             (low_other, col(0, 0)), (low_other, col(1, 0)), (top_other, col(1, 0)), (top_other, col(2, 0)))
        image_own = image_rows(0)
        value = eye(tile) - diag_tiles(image_own, 0, 1)
        store_packed(pd0, 0, value)
        put(d_refs, own, col(1, 0), value)
        for slot in (0, 2):
            value = -diag_tiles(image_own, 0, slot)
            d0[own, col(slot, 0)] = value
            put(d_refs, own, col(slot, 0), value)
        u_diag = [remote(pd0.at[pl.ds(0, 80)], qdn0.at[pl.ds(0, 80)], "u")]
        d_diag = [remote(pd0.at[pl.ds(0, 80)], qup0.at[pl.ds(0, 80)], "d")]
        u_edge = [remote(d0.at[own, col(2, 0)], d0.at[low_own, col(1, 0)], "u")]
        d_edge = [remote(d0.at[own, col(0, 0)], d0.at[top_own, col(1, 0)], "d")]
        sn[other, col(1, 1)] = load_packed(sx, 0)
        load(sn, s_refs, (other, col(1, 1)), (other, col(2, 1)))
        load(z0, z_refs, (other, col(0, 1)), (other, col(2, 1)))

        x_z[1].wait_recv()
        u_z1 = remote(z0.at[other, col(1, 1)], z0.at[low_other, col(0, 1)], "u")
        d_z1 = remote(z0.at[other, col(1, 1)], z0.at[top_other, col(2, 1)], "d")
        start([u_z1] + u_diag + u_edge, [d_z1] + d_diag + d_edge)
        load(z0, z_refs, (other, col(1, 1)))
        receive([u_z2, u_s2, u_s1], [d_z0, d_s1])
        load(z0, z_refs, (low_other, col(1, 1)), (top_other, col(1, 1)))
        sn[other, col(0, 1)] = sx_dn[...].T
        sn[low_other, col(0, 1)] = load_packed(spx_dn, 0)
        sn[top_other, col(2, 1)] = load_packed(spx_up, 0)
        load(sn, s_refs, (other, col(0, 1)), (low_other, col(0, 1)), (top_other, col(2, 1)))
        image_other = image_rows(1)

        def other_rows(slot):
            return sum(nn(image_other[f], near(z_refs, f, slot)) for f in range(3) if abs(f - slot) < 2)

        cross = -diag_tiles(image_own, 1, 1)
        low_part = jnp.concatenate([jnp.zeros((tile, tile), F32), eye(tile)], axis=1) - other_rows(1)
        pd0[pl.ds(80, tile), :] = cross
        store_packed(pd0, 80 + tile, low_part[:, tile:])
        rest = pl.ds(80, tile + 80)
        u_diag.append(remote(pd0.at[rest], qdn0.at[rest], "u"))
        d_diag.append(remote(pd0.at[rest], qup0.at[rest], "d"))
        start(u_diag[1:], d_diag[1:])
        put(d_refs, own, col(1, 1), cross)
        put(d_refs, other, cols(1), low_part)
        receive([u_z1], [d_z1])
        load(z0, z_refs, (low_other, col(0, 1)), (top_other, col(2, 1)))
        for slot in (2, 0):
            cross = -diag_tiles(image_own, 1, slot)
            low_part = -other_rows(slot)
            d0[own, col(slot, 1)] = cross
            d0[other, cols(slot)] = low_part
            if slot == 2:
                u_edge.append(remote(d0.at[own, col(2, 1)], d0.at[low_own, col(1, 1)], "u"))
                u_edge.append(remote(d0.at[other, cols(2)], d0.at[low_other, cols(1)], "u"))
                start(u_edge[1:], [])
            else:
                d_edge.append(remote(d0.at[own, col(0, 1)], d0.at[top_own, col(1, 1)], "d"))
                d_edge.append(remote(d0.at[other, cols(0)], d0.at[top_other, cols(1)], "d"))
                start([], d_edge[1:])
            put(d_refs, own, col(slot, 1), cross)
            put(d_refs, other, cols(slot), low_part)

        for step in range(ITERS):
            last = step == ITERS - 1
            z, d = (z0, d0) if step == 0 else (z1, d1)
            pd, q_dn, q_up = (pd0, qdn0, qup0) if step == 0 else (pd1, qdn1, qup1)

            if step > 0:
                mid = split(z[row1, cols(1)].T)
                t_own = [nn(mid, near(s_refs, 1, 0)), nt(mid, near(s_refs, 1, 1)), nn(mid, near(s_refs, 1, 2))]
                receive(*edge)
                load_split(z, z_refs, ((0, 1), (2, 1)))
                lower = split(z[row0, cols(1)].T)
                upper = split(z[row2, cols(1)].T)
                t = [
                    split(t_own[0] + nn(lower, near(s_refs, 0, 0))),
                    split(t_own[1] + nt(lower, near(s_refs, 1, 0)) + nt(upper, near(s_refs, 1, 2))),
                    split(t_own[2] + nn(upper, near(s_refs, 2, 2))),
                ]
                value = eye(B) - (nn(t[0], near(z_refs, 0, 1)) + nn(t[1], near(z_refs, 1, 1)) + nn(t[2], near(z_refs, 2, 1)))
                store_packed(pd, 0, value[:tile, :tile])
                pd[pl.ds(80, tile), :] = value[:tile, tile:]
                store_packed(pd, 80 + tile, value[tile:, tile:])
                u_diag, d_diag = [remote(pd, q_dn, "u")], [remote(pd, q_up, "d")]
                start(u_diag, d_diag)
                keep_split(d_refs, 1, 1, value)

                receive(ups, dns)
                load_split(z, z_refs, ((0, 0), (2, 2)))
                value = -(nn(t[1], near(z_refs, 1, 2)) + nn(t[2], near(z_refs, 2, 2)))
                d[row1, cols(2)] = value
                u_edge = [remote(d.at[row1, cols(2)], d.at[row0, cols(1)], "u")]
                start(u_edge, [])
                keep_split(d_refs, 1, 2, value)
                value = -(nn(t[0], near(z_refs, 0, 0)) + nn(t[1], near(z_refs, 1, 0)))
                d[row1, cols(0)] = value
                d_edge = [remote(d.at[row1, cols(0)], d.at[row2, cols(1)], "d")]
                start([], d_edge)
                keep_split(d_refs, 1, 0, value)

            mine = own if last else row1
            left = [pick(z_refs, mine, cols(k)) for k in range(3)]
            first = [None, None, None]
            first[1] = sum(nt(left[k], near(d_refs, 1, k)) for k in range(3))
            f_mid = split(first[1])
            second_mid = nt(f_mid, near(d_refs, 1, 1))
            receive(u_diag, d_diag)
            for row, ref in ((0, q_dn), (2, q_up)):
                cross = ref[pl.ds(80, tile), :]
                top = jnp.concatenate([load_packed(ref, 0), cross], axis=1)
                low = jnp.concatenate([cross.T, load_packed(ref, 80 + tile)], axis=1)
                keep_split(d_refs, row, row, jnp.concatenate([top, low], axis=0))
            first[0] = nt(left[0], near(d_refs, 0, 0))
            first[2] = nt(left[2], near(d_refs, 2, 2))
            if step == 0:
                x_k.wait_recv()

            def finish(slot, second):
                value = z[mine, cols(slot)] + 0.5 * first[slot] + 0.375 * second
                for g in range(2):
                    part = value[:tile, g * tile:(g + 1) * tile]
                    if not (slot == 1 and g == 0):
                        part = part * keep_own[2 * slot + g]
                    if last:
                        out_ref[:, pl.ds(pl.multiple_of((2 * slot + half_of(g)) * tile, tile), tile)] = part
                        continue
                    z1[own, col(slot, g)] = part
                    part = value[tile:, g * tile:(g + 1) * tile]
                    if not (slot == 1 and g == 1):
                        r = 2 * slot + 1 - g
                        part = part * kx[r:r + 1, :]
                    z1[other, col(slot, g)] = part

            receive(u_edge, [])
            load_split(d, d_refs, ((0, 1),))
            first[0] = first[0] + nt(left[1], near(d_refs, 0, 1))
            f_low = split(first[0])
            finish(0, nt(f_low, near(d_refs, 0, 0)) + nt(f_mid, near(d_refs, 0, 1)))
            edge = [[], []]
            if not last:
                edge[1].append(remote(z1.at[row1, cols(0)], z1.at[row2, cols(1)], "d"))
                start([], edge[1])
            receive([], d_edge)
            load_split(d, d_refs, ((2, 1),))
            first[2] = first[2] + nt(left[1], near(d_refs, 2, 1))
            f_high = split(first[2])
            finish(2, nt(f_mid, near(d_refs, 2, 1)) + nt(f_high, near(d_refs, 2, 2)))
            if not last:
                edge[0].append(remote(z1.at[row1, cols(2)], z1.at[row0, cols(1)], "u"))
                start(edge[0], [])
            finish(1, second_mid + nt(f_low, near(d_refs, 1, 0)) + nt(f_high, near(d_refs, 1, 2)))
            if not last:
                ups = [remote(z1.at[row1, cols(1)], z1.at[row0, cols(0)], "u")]
                dns = [remote(z1.at[row1, cols(1)], z1.at[row2, cols(2)], "d")]
                start(ups, dns)
                load_split(z1, z_refs, ((1, 0), (1, 1), (1, 2)))

        for c, where in used:
            if where == "x":
                c.wait_send()

        @pl.when(has_up)
        def _():
            for c, where in used:
                if where == "u":
                    c.wait_send()

        @pl.when(has_dn)
        def _():
            for c, where in used:
                if where == "d":
                    c.wait_send()

    return kernel


def solution(mesh):
    n_blk = mesh.shape["blk"]

    def per_device(intersect, half_factors, z_pattern):
        tile = intersect.shape[0]
        near = pltpu.VMEM((3 * B, 3 * B), F32)
        half = pltpu.VMEM((3 * B, 3 * B), BF16)
        block = pltpu.VMEM((tile, tile), F32)
        packed = pltpu.VMEM((80, tile), F32)
        message = pltpu.VMEM((160 + tile, tile), F32)
        return pl.pallas_call(
            make_kernel(n_blk, tile),
            out_shape=jax.ShapeDtypeStruct(intersect.shape, F32),
            in_specs=[
                pl.BlockSpec(memory_space=pltpu.HBM),
                pl.BlockSpec(memory_space=pltpu.HBM),
                pl.BlockSpec(memory_space=pltpu.HBM),
            ],
            out_specs=pl.BlockSpec(memory_space=pltpu.VMEM),
            scratch_shapes=[near] * 5 + [block] * 3 + [packed] * 6 + [message] * 6 + [pltpu.VMEM((8, tile), F32)] * 2 + [half] * 6

            + [pltpu.SMEM((1, 6), jnp.int32), pltpu.SemaphoreType.DMA((10,)), pltpu.SemaphoreType.DMA((48,)), pltpu.SemaphoreType.DMA((48,))],
            compiler_params=pltpu.CompilerParams(
                collective_id=0, has_side_effects=True, vmem_limit_bytes=48 * 1024 * 1024),
            name="merge",
        )(intersect, half_factors, z_pattern)

    spec = P(("pair", "side", "blk"), None)
    return jax.shard_map(per_device, mesh=mesh, in_specs=(spec,) * 3, out_specs=spec, check_vma=False)
```

```python
import jax
import jax.numpy as jnp
from jax import lax
from jax.experimental import pallas as pl
from jax.experimental.pallas import tpu as pltpu
from jax.sharding import PartitionSpec as P

ITERS = 2
MESH = pl.DeviceIdType.MESH
F32 = jnp.float32
BF16 = jnp.bfloat16
B = 256


def split(value):
    high = value.astype(BF16)
    low = (value - high.astype(F32)).astype(BF16)
    return high, low


def lanes(shape):
    return lax.broadcasted_iota(jnp.int32, shape, 1)


def store_packed(ref, start, tile):
    ref[pl.ds(start, 32), :] = tile[0:32]
    ref[pl.ds(start + 32, 32), :] = jnp.where(lanes((32, 128)) < 32, pltpu.roll(tile[96:128], 32, 1), tile[32:64])
    ref[pl.ds(start + 64, 16), :] = jnp.where(lanes((16, 128)) < 64, pltpu.roll(tile[80:96], 64, 1), tile[64:80])


def load_packed(ref, start):
    first = ref[pl.ds(start, 32), :]
    second = ref[pl.ds(start + 32, 32), :]
    third = ref[pl.ds(start + 64, 16), :]
    upper = jnp.concatenate(
        [first, second, third, pltpu.roll(third, 64, 1), pltpu.roll(second, 96, 1)], axis=0)
    row = lax.broadcasted_iota(jnp.int32, (128, 128), 0)
    return jnp.where(lanes((128, 128)) >= row, upper, upper.T)


def dot3(left, right, nt):
    dims = (((1,), (1 if nt else 0,)), ((), ()))

    def one(x, y):
        return lax.dot_general(x, y, dims, preferred_element_type=F32)

    return one(left[0], right[0]) + one(left[0], right[1]) + one(left[1], right[0])


def make_kernel(n_blk, tile):
    own = pl.ds(B, tile)
    other = pl.ds(B + tile, tile)
    row0, row1, row2 = pl.ds(0, B), pl.ds(B, B), pl.ds(2 * B, B)
    rows_of = (row0, row1, row2)
    low_own, low_other = pl.ds(0, tile), pl.ds(tile, tile)
    top_own, top_other = pl.ds(2 * B, tile), pl.ds(2 * B + tile, tile)

    def col(slot, half):
        return pl.ds(slot * B + half * tile, tile)

    def cols(slot):
        return pl.ds(slot * B, B)

    def kernel(s_hbm, h_hbm, zp_hbm, out_ref, sn, z0, z1, d0, d1, so_dn, so_up, sx_dn, sp, sx, spo_dn, spo_up, spx_dn, spx_up,
               pd0, pd1, qdn0, qdn1, qup0, qup1, kbuf, kx,
               s_hi, s_lo, z_hi, z_lo, d_hi, d_lo, zp_ref, lsem, ssem, rsem):
        side = lax.axis_index("side")
        blk = lax.axis_index("blk")
        partner = {"side": 1 - side}
        up = {"blk": blk + 1}
        dn = {"blk": blk - 1}
        has_up = blk < n_blk - 1
        has_dn = blk > 0

        barrier = pltpu.get_barrier_semaphore()
        pl.semaphore_signal(barrier, inc=1, device_id=partner, device_id_type=MESH)

        @pl.when(has_up)
        def _():
            pl.semaphore_signal(barrier, inc=1, device_id=up, device_id_type=MESH)

        @pl.when(has_dn)
        def _():
            pl.semaphore_signal(barrier, inc=1, device_id=dn, device_id_type=MESH)

        def half_of(g):
            return side if g == 0 else 1 - side

        h_loads = [
            pltpu.make_async_copy(h_hbm.at[:, pl.ds(e * tile, tile)], z0.at[own, col(e, 0)], lsem.at[6 + e])
            for e in range(3)
        ]
        s_loads = []
        for e in range(3):
            for g in range(2):
                src = s_hbm.at[:, pl.ds(pl.multiple_of((2 * e + half_of(g)) * tile, tile), tile)]
                s_loads.append(pltpu.make_async_copy(src, sn.at[own, col(e, g)], lsem.at[2 * e + g]))
        zp_load = pltpu.make_async_copy(zp_hbm, zp_ref, lsem.at[9])
        for load in h_loads + s_loads + [zp_load]:
            load.start()
        for load in h_loads + s_loads:
            load.wait()

        inner = jnp.logical_and(has_up, has_dn)

        @pl.when(inner)
        def _():
            pl.semaphore_wait(barrier, 3)

        @pl.when(jnp.logical_not(inner))
        def _():
            pl.semaphore_wait(barrier, 2)

        used = []

        def remote(src, dst, where):
            i = len(used)
            copy = pltpu.make_async_remote_copy(
                src_ref=src, dst_ref=dst, send_sem=ssem.at[i], recv_sem=rsem.at[i],
                device_id={"x": partner, "u": up, "d": dn}[where], device_id_type=MESH)
            used.append((copy, where))
            return copy

        def start(ups, dns):
            if ups:
                @pl.when(has_up)
                def _():
                    for c in ups:
                        c.start()
            if dns:
                @pl.when(has_dn)
                def _():
                    for c in dns:
                        c.start()

        def receive(ups, dns):
            if ups:
                @pl.when(has_dn)
                def _():
                    for c in ups:
                        c.wait_recv()
            if dns:
                @pl.when(has_up)
                def _():
                    for c in dns:
                        c.wait_recv()

        x_z = [remote(z0.at[own, col(e, 0)], z0.at[other, col(e, 1)], "x") for e in range(3)]
        x_s1 = remote(sp, sx, "x")
        x_s2 = remote(sn.at[own, col(2, 0)], sn.at[other, col(2, 1)], "x")
        x_k = remote(kbuf, kx, "x")
        for c in (x_z[0], x_z[2], x_s2):
            c.start()
        store_packed(sp, 0, sn[own, col(1, 0)])
        x_s1.start()
        x_z[1].start()

        u_own = [
            remote(z0.at[own, col(2, 0)], z0.at[low_own, col(1, 0)], "u"),
            remote(sp, spo_dn, "u"),
            remote(sn.at[own, col(1, 1)], sn.at[low_own, col(0, 1)], "u"),
            remote(sn.at[own, col(2, 1)], so_dn, "u"),
            remote(z0.at[own, col(1, 0)], z0.at[low_own, col(0, 0)], "u"),
        ]
        d_own = [
            remote(z0.at[own, col(0, 0)], z0.at[top_own, col(1, 0)], "d"),
            remote(sp, spo_up, "d"),
            remote(sn.at[own, col(1, 1)], sn.at[top_own, col(2, 1)], "d"),
            remote(sn.at[own, col(0, 1)], so_up, "d"),
            remote(z0.at[own, col(1, 0)], z0.at[top_own, col(2, 0)], "d"),
        ]
        start(u_own, d_own)

        zp_load.wait()
        keep_own = [zp_ref[0, 2 * e + half_of(g)].astype(F32) for e in range(3) for g in range(2)]
        row_id = lax.broadcasted_iota(jnp.int32, (8, tile), 0)
        packed = jnp.zeros((8, tile), F32)
        for r in range(6):
            packed = jnp.where(row_id == r, keep_own[r], packed)
        kbuf[...] = packed

        zero = jnp.zeros((tile, tile), F32)
        for e in range(3):
            z0[own, col(e, 1)] = zero
            z0[other, col(e, 0)] = zero
        for e in (0, 1):
            z0[low_own, col(e, 1)] = zero
            z0[low_other, col(e, 0)] = zero
            z0[top_own, col(e + 1, 1)] = zero
            z0[top_other, col(e + 1, 0)] = zero

        @pl.when(jnp.logical_not(has_dn))
        def _():
            for e in (0, 1):
                z0[low_own, col(e, 0)] = zero
                z0[low_other, col(e, 1)] = zero
                z1[row0, cols(e)] = jnp.zeros((B, B), F32)
            for ref in (d0, d1):
                ref[row0, cols(1)] = jnp.zeros((B, B), F32)
            for ref in (spo_dn, spx_dn, qdn0, qdn1):
                ref[...] = jnp.zeros(ref.shape, F32)
            sn[low_own, col(0, 1)] = zero
            so_dn[...] = zero
            sx_dn[...] = zero

        @pl.when(jnp.logical_not(has_up))
        def _():
            for e in (1, 2):
                z0[top_own, col(e, 0)] = zero
                z0[top_other, col(e, 1)] = zero
                z1[row2, cols(e)] = jnp.zeros((B, B), F32)
            for ref in (d0, d1):
                ref[row2, cols(1)] = jnp.zeros((B, B), F32)
            for ref in (spo_up, spx_up, qup0, qup1):
                ref[...] = jnp.zeros(ref.shape, F32)
            sn[top_own, col(2, 1)] = zero
            so_up[...] = zero

        x_k.start()

        s_refs, z_refs, d_refs = (s_hi, s_lo), (z_hi, z_lo), (d_hi, d_lo)

        def keep_split(refs, row, slot, value):
            high, low = split(value)
            refs[0][rows_of[row], cols(slot)] = high
            refs[1][rows_of[row], cols(slot)] = low

        def load_split(ref, refs, places):
            for row, slot in places:
                keep_split(refs, row, slot, ref[rows_of[row], cols(slot)])

        def pick(refs, rows, columns):
            return refs[0][rows, columns], refs[1][rows, columns]

        def near(refs, row, slot):
            return pick(refs, rows_of[row], cols(slot))

        def nn(left, right):
            return dot3(left, right, False)

        def nt(left, right):
            return dot3(left, right, True)

        low_rows, mid_rows, top_rows = (low_own, low_other), (own, other), (top_own, top_other)

        def load(ref, refs, *places):
            for rows, columns in places:
                high, low = split(ref[rows, columns])
                refs[0][rows, columns] = high
                refs[1][rows, columns] = low

        def put(refs, rows, columns, value):
            high, low = split(value)
            refs[0][rows, columns] = high
            refs[1][rows, columns] = low

        def eye(n):
            return (lax.broadcasted_iota(jnp.int32, (n, n), 0) == lax.broadcasted_iota(jnp.int32, (n, n), 1)).astype(F32)

        def image_rows(h):
            mid = split(z0[mid_rows[h], col(1, h)].T)
            lower = split(z0[low_rows[h], col(1, h)].T)
            upper = split(z0[top_rows[h], col(1, h)].T)
            here = [pick(s_refs, mid_rows[h], cols(k)) for k in range(3)]
            return [
                split(nn(lower, pick(s_refs, low_rows[h], cols(0))) + nn(mid, here[0])),
                split(nt(lower, pick(s_refs, row1, col(0, h))) + nn(mid, here[1]) + nt(upper, pick(s_refs, row1, col(2, h)))),
                split(nn(mid, here[2]) + nn(upper, pick(s_refs, top_rows[h], cols(2)))),
            ]

        def half_cols(pair, h):
            return pair[0][:, h * tile:(h + 1) * tile], pair[1][:, h * tile:(h + 1) * tile]

        def diag_tiles(image, h, slot):
            near_rows = (low_rows[h], mid_rows[h], top_rows[h])
            return sum(nn(half_cols(image[f], h), pick(z_refs, near_rows[f], col(slot, h)))
                       for f in range(3) if abs(f - slot) < 2)

        sn[other, col(1, 0)] = sn[own, col(1, 1)].T
        load(sn, s_refs, (own, cols(0)), (own, cols(1)), (own, cols(2)), (other, col(1, 0)))
        load(z0, z_refs, *[(own, cols(e)) for e in range(3)], *[(other, col(e, 0)) for e in range(3)])
        x_z[0].wait_recv()
        d_z0 = remote(z0.at[other, col(0, 1)], z0.at[top_other, col(1, 1)], "d")
        start([], [d_z0])
        x_z[2].wait_recv()
        u_z2 = remote(z0.at[other, col(2, 1)], z0.at[low_other, col(1, 1)], "u")
        start([u_z2], [])
        x_s2.wait_recv()
        u_s2 = remote(sn.at[other, col(2, 1)], sx_dn, "u")
        start([u_s2], [])
        x_s1.wait_recv()
        u_s1 = remote(sx, spx_dn, "u")
        d_s1 = remote(sx, spx_up, "d")
        start([u_s1], [d_s1])

        receive(u_own, d_own)
        sn[other, col(0, 0)] = so_dn[...].T
        sn[other, col(2, 0)] = so_up[...].T
        sn[low_own, col(0, 0)] = load_packed(spo_dn, 0)
        sn[top_own, col(2, 0)] = load_packed(spo_up, 0)
        sn[low_other, col(0, 0)] = sn[low_own, col(0, 1)].T
        sn[top_other, col(2, 0)] = sn[top_own, col(2, 1)].T
        load(sn, s_refs, (low_own, cols(0)), (top_own, cols(2)), (other, col(0, 0)), (other, col(2, 0)),
             (low_other, col(0, 0)), (top_other, col(2, 0)))
        load(z0, z_refs, (low_own, cols(0)), (low_own, cols(1)), (top_own, cols(1)), (top_own, cols(2)),
             (low_other, col(0, 0)), (low_other, col(1, 0)), (top_other, col(1, 0)), (top_other, col(2, 0)))
        image_own = image_rows(0)
        value = eye(tile) - diag_tiles(image_own, 0, 1)
        store_packed(pd0, 0, value)
        put(d_refs, own, col(1, 0), value)
        for slot in (0, 2):
            value = -diag_tiles(image_own, 0, slot)
            d0[own, col(slot, 0)] = value
            put(d_refs, own, col(slot, 0), value)
        u_diag = [remote(pd0.at[pl.ds(0, 80)], qdn0.at[pl.ds(0, 80)], "u")]
        d_diag = [remote(pd0.at[pl.ds(0, 80)], qup0.at[pl.ds(0, 80)], "d")]
        u_edge = [remote(d0.at[own, col(2, 0)], d0.at[low_own, col(1, 0)], "u")]
        d_edge = [remote(d0.at[own, col(0, 0)], d0.at[top_own, col(1, 0)], "d")]
        sn[other, col(1, 1)] = load_packed(sx, 0)
        load(sn, s_refs, (other, col(1, 1)), (other, col(2, 1)))
        load(z0, z_refs, (other, col(0, 1)), (other, col(2, 1)))

        x_z[1].wait_recv()
        u_z1 = remote(z0.at[other, col(1, 1)], z0.at[low_other, col(0, 1)], "u")
        d_z1 = remote(z0.at[other, col(1, 1)], z0.at[top_other, col(2, 1)], "d")
        start([u_z1] + u_diag + u_edge, [d_z1] + d_diag + d_edge)
        load(z0, z_refs, (other, col(1, 1)))
        receive([u_z2, u_s2, u_s1], [d_z0, d_s1])
        load(z0, z_refs, (low_other, col(1, 1)), (top_other, col(1, 1)))
        sn[other, col(0, 1)] = sx_dn[...].T
        sn[low_other, col(0, 1)] = load_packed(spx_dn, 0)
        sn[top_other, col(2, 1)] = load_packed(spx_up, 0)
        load(sn, s_refs, (other, col(0, 1)), (low_other, col(0, 1)), (top_other, col(2, 1)))
        image_other = image_rows(1)

        def other_rows(slot):
            return sum(nn(image_other[f], near(z_refs, f, slot)) for f in range(3) if abs(f - slot) < 2)

        cross = -diag_tiles(image_own, 1, 1)
        low_part = jnp.concatenate([jnp.zeros((tile, tile), F32), eye(tile)], axis=1) - other_rows(1)
        pd0[pl.ds(80, tile), :] = cross
        store_packed(pd0, 80 + tile, low_part[:, tile:])
        rest = pl.ds(80, tile + 80)
        u_diag.append(remote(pd0.at[rest], qdn0.at[rest], "u"))
        d_diag.append(remote(pd0.at[rest], qup0.at[rest], "d"))
        start(u_diag[1:], d_diag[1:])
        put(d_refs, own, col(1, 1), cross)
        put(d_refs, other, cols(1), low_part)
        part = {}
        for slot in (2, 0):
            part[slot] = (nn(half_cols(image_own[1], 1), pick(z_refs, other, col(slot, 1))),
                          nn(image_other[1], near(z_refs, 1, slot)))
        receive([u_z1], [d_z1])
        load(z0, z_refs, (low_other, col(0, 1)), (top_other, col(2, 1)))
        edges = {}
        for slot, rows in ((2, top_other), (0, low_other)):
            cross = -(part[slot][0] + nn(half_cols(image_own[slot], 1), pick(z_refs, rows, col(slot, 1))))
            low_part = -(part[slot][1] + nn(image_other[slot], near(z_refs, slot, slot)))
            d0[own, col(slot, 1)] = cross
            d0[other, cols(slot)] = low_part
            edges[slot] = cross, low_part
        u_edge.append(remote(d0.at[own, col(2, 1)], d0.at[low_own, col(1, 1)], "u"))
        u_edge.append(remote(d0.at[other, cols(2)], d0.at[low_other, cols(1)], "u"))
        d_edge.append(remote(d0.at[own, col(0, 1)], d0.at[top_own, col(1, 1)], "d"))
        d_edge.append(remote(d0.at[other, cols(0)], d0.at[top_other, cols(1)], "d"))
        start(u_edge[1:], d_edge[1:])
        for slot in (2, 0):
            put(d_refs, own, col(slot, 1), edges[slot][0])
            put(d_refs, other, cols(slot), edges[slot][1])

        for step in range(ITERS):
            last = step == ITERS - 1
            z, d = (z0, d0) if step == 0 else (z1, d1)
            pd, q_dn, q_up = (pd0, qdn0, qup0) if step == 0 else (pd1, qdn1, qup1)

            if step > 0:
                mid = split(z[row1, cols(1)].T)
                t_own = [nn(mid, near(s_refs, 1, 0)), nt(mid, near(s_refs, 1, 1)), nn(mid, near(s_refs, 1, 2))]
                receive(*edge)
                load_split(z, z_refs, ((0, 1), (2, 1)))
                lower = split(z[row0, cols(1)].T)
                upper = split(z[row2, cols(1)].T)
                t = [
                    split(t_own[0] + nn(lower, near(s_refs, 0, 0))),
                    split(t_own[1] + nt(lower, near(s_refs, 1, 0)) + nt(upper, near(s_refs, 1, 2))),
                    split(t_own[2] + nn(upper, near(s_refs, 2, 2))),
                ]
                value = eye(B) - (nn(t[0], near(z_refs, 0, 1)) + nn(t[1], near(z_refs, 1, 1)) + nn(t[2], near(z_refs, 2, 1)))
                store_packed(pd, 0, value[:tile, :tile])
                pd[pl.ds(80, tile), :] = value[:tile, tile:]
                store_packed(pd, 80 + tile, value[tile:, tile:])
                u_diag, d_diag = [remote(pd, q_dn, "u")], [remote(pd, q_up, "d")]
                start(u_diag, d_diag)
                keep_split(d_refs, 1, 1, value)

                part_up, part_dn = nn(t[1], near(z_refs, 1, 2)), nn(t[1], near(z_refs, 1, 0))
                receive(ups, dns)
                load_split(z, z_refs, ((0, 0), (2, 2)))
                value_up = -(part_up + nn(t[2], near(z_refs, 2, 2)))
                value_dn = -(part_dn + nn(t[0], near(z_refs, 0, 0)))
                d[row1, cols(2)] = value_up
                d[row1, cols(0)] = value_dn
                u_edge = [remote(d.at[row1, cols(2)], d.at[row0, cols(1)], "u")]
                d_edge = [remote(d.at[row1, cols(0)], d.at[row2, cols(1)], "d")]
                start(u_edge, d_edge)
                keep_split(d_refs, 1, 2, value_up)
                keep_split(d_refs, 1, 0, value_dn)

            mine = own if last else row1
            left = [pick(z_refs, mine, cols(k)) for k in range(3)]
            first = [None, None, None]
            first[1] = sum(nt(left[k], near(d_refs, 1, k)) for k in range(3))
            f_mid = split(first[1])
            second_mid = nt(f_mid, near(d_refs, 1, 1))
            receive(u_diag, d_diag)
            for row, ref in ((0, q_dn), (2, q_up)):
                cross = ref[pl.ds(80, tile), :]
                top = jnp.concatenate([load_packed(ref, 0), cross], axis=1)
                low = jnp.concatenate([cross.T, load_packed(ref, 80 + tile)], axis=1)
                keep_split(d_refs, row, row, jnp.concatenate([top, low], axis=0))
            first[0] = nt(left[0], near(d_refs, 0, 0))
            first[2] = nt(left[2], near(d_refs, 2, 2))
            if step == 0:
                x_k.wait_recv()

            def finish(slot, second):
                value = z[mine, cols(slot)] + 0.5 * first[slot] + 0.375 * second
                for g in range(2):
                    part = value[:tile, g * tile:(g + 1) * tile]
                    if not (slot == 1 and g == 0):
                        part = part * keep_own[2 * slot + g]
                    if last:
                        out_ref[:, pl.ds(pl.multiple_of((2 * slot + half_of(g)) * tile, tile), tile)] = part
                        continue
                    z1[own, col(slot, g)] = part
                    part = value[tile:, g * tile:(g + 1) * tile]
                    if not (slot == 1 and g == 1):
                        r = 2 * slot + 1 - g
                        part = part * kx[r:r + 1, :]
                    z1[other, col(slot, g)] = part

            receive(u_edge, d_edge)
            load_split(d, d_refs, ((0, 1), (2, 1)))
            first[0] = first[0] + nt(left[1], near(d_refs, 0, 1))
            first[2] = first[2] + nt(left[1], near(d_refs, 2, 1))
            f_low, f_high = split(first[0]), split(first[2])
            finish(0, nt(f_low, near(d_refs, 0, 0)) + nt(f_mid, near(d_refs, 0, 1)))
            finish(2, nt(f_high, near(d_refs, 2, 2)) + nt(f_mid, near(d_refs, 2, 1)))
            edge = [[], []]
            if not last:
                edge[0].append(remote(z1.at[row1, cols(2)], z1.at[row0, cols(1)], "u"))
                edge[1].append(remote(z1.at[row1, cols(0)], z1.at[row2, cols(1)], "d"))
                start(*edge)
            finish(1, second_mid + nt(f_low, near(d_refs, 1, 0)) + nt(f_high, near(d_refs, 1, 2)))
            if not last:
                ups = [remote(z1.at[row1, cols(1)], z1.at[row0, cols(0)], "u")]
                dns = [remote(z1.at[row1, cols(1)], z1.at[row2, cols(2)], "d")]
                start(ups, dns)
                load_split(z1, z_refs, ((1, 0), (1, 1), (1, 2)))

        for c, where in used:
            if where == "x":
                c.wait_send()

        @pl.when(has_up)
        def _():
            for c, where in used:
                if where == "u":
                    c.wait_send()

        @pl.when(has_dn)
        def _():
            for c, where in used:
                if where == "d":
                    c.wait_send()

    return kernel


def solution(mesh):
    n_blk = mesh.shape["blk"]

    def per_device(intersect, half_factors, z_pattern):
        tile = intersect.shape[0]
        near = pltpu.VMEM((3 * B, 3 * B), F32)
        half = pltpu.VMEM((3 * B, 3 * B), BF16)
        block = pltpu.VMEM((tile, tile), F32)
        packed = pltpu.VMEM((80, tile), F32)
        message = pltpu.VMEM((160 + tile, tile), F32)
        return pl.pallas_call(
            make_kernel(n_blk, tile),
            out_shape=jax.ShapeDtypeStruct(intersect.shape, F32),
            in_specs=[
                pl.BlockSpec(memory_space=pltpu.HBM),
                pl.BlockSpec(memory_space=pltpu.HBM),
                pl.BlockSpec(memory_space=pltpu.HBM),
            ],
            out_specs=pl.BlockSpec(memory_space=pltpu.VMEM),
            scratch_shapes=[near] * 5 + [block] * 3 + [packed] * 6 + [message] * 6 + [pltpu.VMEM((8, tile), F32)] * 2 + [half] * 6

            + [pltpu.SMEM((1, 6), jnp.int32), pltpu.SemaphoreType.DMA((10,)), pltpu.SemaphoreType.DMA((48,)), pltpu.SemaphoreType.DMA((48,))],
            compiler_params=pltpu.CompilerParams(
                collective_id=0, has_side_effects=True, vmem_limit_bytes=48 * 1024 * 1024),
            name="merge",
        )(intersect, half_factors, z_pattern)

    spec = P(("pair", "side", "blk"), None)
    return jax.shard_map(per_device, mesh=mesh, in_specs=(spec,) * 3, out_specs=spec, check_vma=False)
```

```python
import jax
import jax.numpy as jnp
from jax import lax
from jax.experimental import pallas as pl
from jax.experimental.pallas import tpu as pltpu
from jax.sharding import PartitionSpec as P

ITERS = 2
MESH = pl.DeviceIdType.MESH
F32 = jnp.float32
BF16 = jnp.bfloat16
B = 256


def split(value):
    high = value.astype(BF16)
    low = (value - high.astype(F32)).astype(BF16)
    return high, low


def lanes(shape):
    return lax.broadcasted_iota(jnp.int32, shape, 1)


def store_packed(ref, start, tile):
    ref[pl.ds(start, 32), :] = tile[0:32]
    ref[pl.ds(start + 32, 32), :] = jnp.where(lanes((32, 128)) < 32, pltpu.roll(tile[96:128], 32, 1), tile[32:64])
    ref[pl.ds(start + 64, 16), :] = jnp.where(lanes((16, 128)) < 64, pltpu.roll(tile[80:96], 64, 1), tile[64:80])


def load_packed(ref, start):
    first = ref[pl.ds(start, 32), :]
    second = ref[pl.ds(start + 32, 32), :]
    third = ref[pl.ds(start + 64, 16), :]
    upper = jnp.concatenate(
        [first, second, third, pltpu.roll(third, 64, 1), pltpu.roll(second, 96, 1)], axis=0)
    row = lax.broadcasted_iota(jnp.int32, (128, 128), 0)
    return jnp.where(lanes((128, 128)) >= row, upper, upper.T)


def dot3(left, right, nt):
    dims = (((1,), (1 if nt else 0,)), ((), ()))

    def one(x, y):
        return lax.dot_general(x, y, dims, preferred_element_type=F32)

    return one(left[0], right[0]) + one(left[0], right[1]) + one(left[1], right[0])


def make_kernel(n_blk, tile):
    own = pl.ds(B, tile)
    other = pl.ds(B + tile, tile)
    row0, row1, row2 = pl.ds(0, B), pl.ds(B, B), pl.ds(2 * B, B)
    rows_of = (row0, row1, row2)
    low_own, low_other = pl.ds(0, tile), pl.ds(tile, tile)
    top_own, top_other = pl.ds(2 * B, tile), pl.ds(2 * B + tile, tile)

    def col(slot, half):
        return pl.ds(slot * B + half * tile, tile)

    def cols(slot):
        return pl.ds(slot * B, B)

    def kernel(s_hbm, h_hbm, zp_hbm, out_ref, sn, z0, z1, d0, d1, so_dn, so_up, sx_dn, sp, sx, spo_dn, spo_up, spx_dn, spx_up,
               pd0, pd1, qdn0, qdn1, qup0, qup1, kbuf, kx,
               s_hi, s_lo, z_hi, z_lo, d_hi, d_lo, zp_ref, lsem, ssem, rsem):
        side = lax.axis_index("side")
        blk = lax.axis_index("blk")
        partner = {"side": 1 - side}
        up = {"blk": blk + 1}
        dn = {"blk": blk - 1}
        has_up = blk < n_blk - 1
        has_dn = blk > 0

        barrier = pltpu.get_barrier_semaphore()
        pl.semaphore_signal(barrier, inc=1, device_id=partner, device_id_type=MESH)

        @pl.when(has_up)
        def _():
            pl.semaphore_signal(barrier, inc=1, device_id=up, device_id_type=MESH)

        @pl.when(has_dn)
        def _():
            pl.semaphore_signal(barrier, inc=1, device_id=dn, device_id_type=MESH)

        def half_of(g):
            return side if g == 0 else 1 - side

        h_loads = [
            pltpu.make_async_copy(h_hbm.at[:, pl.ds(e * tile, tile)], z0.at[own, col(e, 0)], lsem.at[6 + e])
            for e in range(3)
        ]
        s_loads = []
        for e in range(3):
            for g in range(2):
                src = s_hbm.at[:, pl.ds(pl.multiple_of((2 * e + half_of(g)) * tile, tile), tile)]
                s_loads.append(pltpu.make_async_copy(src, sn.at[own, col(e, g)], lsem.at[2 * e + g]))
        zp_load = pltpu.make_async_copy(zp_hbm, zp_ref, lsem.at[9])
        for load in h_loads + s_loads + [zp_load]:
            load.start()
        for load in h_loads + s_loads:
            load.wait()

        inner = jnp.logical_and(has_up, has_dn)

        @pl.when(inner)
        def _():
            pl.semaphore_wait(barrier, 3)

        @pl.when(jnp.logical_not(inner))
        def _():
            pl.semaphore_wait(barrier, 2)

        used = []

        def remote(src, dst, where):
            i = len(used)
            copy = pltpu.make_async_remote_copy(
                src_ref=src, dst_ref=dst, send_sem=ssem.at[i], recv_sem=rsem.at[i],
                device_id={"x": partner, "u": up, "d": dn}[where], device_id_type=MESH)
            used.append((copy, where))
            return copy

        def start(ups, dns):
            if ups:
                @pl.when(has_up)
                def _():
                    for c in ups:
                        c.start()
            if dns:
                @pl.when(has_dn)
                def _():
                    for c in dns:
                        c.start()

        def receive(ups, dns):
            if ups:
                @pl.when(has_dn)
                def _():
                    for c in ups:
                        c.wait_recv()
            if dns:
                @pl.when(has_up)
                def _():
                    for c in dns:
                        c.wait_recv()

        x_z = [remote(z0.at[own, col(e, 0)], z0.at[other, col(e, 1)], "x") for e in range(3)]
        x_s1 = remote(sp, sx, "x")
        x_s2 = remote(sn.at[own, col(2, 0)], sn.at[other, col(2, 1)], "x")
        x_k = remote(kbuf, kx, "x")
        store_packed(sp, 0, sn[own, col(1, 0)])
        for c in (x_z[0], x_z[2], x_s2):
            c.start()

        u_own = [
            remote(z0.at[own, col(2, 0)], z0.at[low_own, col(1, 0)], "u"),
            remote(sp, spo_dn, "u"),
            remote(sn.at[own, col(1, 1)], sn.at[low_own, col(0, 1)], "u"),
            remote(sn.at[own, col(2, 1)], so_dn, "u"),
            remote(z0.at[own, col(1, 0)], z0.at[low_own, col(0, 0)], "u"),
        ]
        d_own = [
            remote(z0.at[own, col(0, 0)], z0.at[top_own, col(1, 0)], "d"),
            remote(sp, spo_up, "d"),
            remote(sn.at[own, col(1, 1)], sn.at[top_own, col(2, 1)], "d"),
            remote(sn.at[own, col(0, 1)], so_up, "d"),
            remote(z0.at[own, col(1, 0)], z0.at[top_own, col(2, 0)], "d"),
        ]
        start(u_own, d_own)
        for c in (x_s1, x_z[1]):
            c.start()

        zp_load.wait()
        keep_own = [zp_ref[0, 2 * e + half_of(g)].astype(F32) for e in range(3) for g in range(2)]
        row_id = lax.broadcasted_iota(jnp.int32, (8, tile), 0)
        packed = jnp.zeros((8, tile), F32)
        for r in range(6):
            packed = jnp.where(row_id == r, keep_own[r], packed)
        kbuf[...] = packed

        zero = jnp.zeros((tile, tile), F32)
        for e in range(3):
            z0[own, col(e, 1)] = zero
            z0[other, col(e, 0)] = zero
        for e in (0, 1):
            z0[low_own, col(e, 1)] = zero
            z0[low_other, col(e, 0)] = zero
            z0[top_own, col(e + 1, 1)] = zero
            z0[top_other, col(e + 1, 0)] = zero

        @pl.when(jnp.logical_not(has_dn))
        def _():
            for e in (0, 1):
                z0[low_own, col(e, 0)] = zero
                z0[low_other, col(e, 1)] = zero
                z1[row0, cols(e)] = jnp.zeros((B, B), F32)
            for ref in (d0, d1):
                ref[row0, cols(1)] = jnp.zeros((B, B), F32)
            for ref in (spo_dn, spx_dn, qdn0, qdn1):
                ref[...] = jnp.zeros(ref.shape, F32)
            sn[low_own, col(0, 1)] = zero
            so_dn[...] = zero
            sx_dn[...] = zero

        @pl.when(jnp.logical_not(has_up))
        def _():
            for e in (1, 2):
                z0[top_own, col(e, 0)] = zero
                z0[top_other, col(e, 1)] = zero
                z1[row2, cols(e)] = jnp.zeros((B, B), F32)
            for ref in (d0, d1):
                ref[row2, cols(1)] = jnp.zeros((B, B), F32)
            for ref in (spo_up, spx_up, qup0, qup1):
                ref[...] = jnp.zeros(ref.shape, F32)
            sn[top_own, col(2, 1)] = zero
            so_up[...] = zero

        x_k.start()

        s_refs, z_refs, d_refs = (s_hi, s_lo), (z_hi, z_lo), (d_hi, d_lo)

        def keep_split(refs, row, slot, value):
            high, low = split(value)
            refs[0][rows_of[row], cols(slot)] = high
            refs[1][rows_of[row], cols(slot)] = low

        def load_split(ref, refs, places):
            for row, slot in places:
                keep_split(refs, row, slot, ref[rows_of[row], cols(slot)])

        def pick(refs, rows, columns):
            return refs[0][rows, columns], refs[1][rows, columns]

        def near(refs, row, slot):
            return pick(refs, rows_of[row], cols(slot))

        def nn(left, right):
            return dot3(left, right, False)

        def nt(left, right):
            return dot3(left, right, True)

        low_rows, mid_rows, top_rows = (low_own, low_other), (own, other), (top_own, top_other)

        def load(ref, refs, *places):
            for rows, columns in places:
                high, low = split(ref[rows, columns])
                refs[0][rows, columns] = high
                refs[1][rows, columns] = low

        def put(refs, rows, columns, value):
            high, low = split(value)
            refs[0][rows, columns] = high
            refs[1][rows, columns] = low

        def eye(n):
            return (lax.broadcasted_iota(jnp.int32, (n, n), 0) == lax.broadcasted_iota(jnp.int32, (n, n), 1)).astype(F32)

        def image_rows(h):
            mid = split(z0[mid_rows[h], col(1, h)].T)
            lower = split(z0[low_rows[h], col(1, h)].T)
            upper = split(z0[top_rows[h], col(1, h)].T)
            here = [pick(s_refs, mid_rows[h], cols(k)) for k in range(3)]
            return [
                split(nn(lower, pick(s_refs, low_rows[h], cols(0))) + nn(mid, here[0])),
                split(nt(lower, pick(s_refs, row1, col(0, h))) + nn(mid, here[1]) + nt(upper, pick(s_refs, row1, col(2, h)))),
                split(nn(mid, here[2]) + nn(upper, pick(s_refs, top_rows[h], cols(2)))),
            ]

        def half_cols(pair, h):
            return pair[0][:, h * tile:(h + 1) * tile], pair[1][:, h * tile:(h + 1) * tile]

        def diag_tiles(image, h, slot):
            near_rows = (low_rows[h], mid_rows[h], top_rows[h])
            return sum(nn(half_cols(image[f], h), pick(z_refs, near_rows[f], col(slot, h)))
                       for f in range(3) if abs(f - slot) < 2)

        sn[other, col(1, 0)] = sn[own, col(1, 1)].T
        load(sn, s_refs, (own, cols(0)), (own, cols(1)), (own, cols(2)), (other, col(1, 0)))
        load(z0, z_refs, *[(own, cols(e)) for e in range(3)], *[(other, col(e, 0)) for e in range(3)])
        x_z[0].wait_recv()
        d_z0 = remote(z0.at[other, col(0, 1)], z0.at[top_other, col(1, 1)], "d")
        start([], [d_z0])
        x_z[2].wait_recv()
        u_z2 = remote(z0.at[other, col(2, 1)], z0.at[low_other, col(1, 1)], "u")
        start([u_z2], [])
        x_s2.wait_recv()
        u_s2 = remote(sn.at[other, col(2, 1)], sx_dn, "u")
        start([u_s2], [])
        x_s1.wait_recv()
        u_s1 = remote(sx, spx_dn, "u")
        d_s1 = remote(sx, spx_up, "d")
        start([u_s1], [d_s1])

        receive(u_own, d_own)
        sn[other, col(0, 0)] = so_dn[...].T
        sn[other, col(2, 0)] = so_up[...].T
        sn[low_own, col(0, 0)] = load_packed(spo_dn, 0)
        sn[top_own, col(2, 0)] = load_packed(spo_up, 0)
        sn[low_other, col(0, 0)] = sn[low_own, col(0, 1)].T
        sn[top_other, col(2, 0)] = sn[top_own, col(2, 1)].T
        load(sn, s_refs, (low_own, cols(0)), (top_own, cols(2)), (other, col(0, 0)), (other, col(2, 0)),
             (low_other, col(0, 0)), (top_other, col(2, 0)))
        load(z0, z_refs, (low_own, cols(0)), (low_own, cols(1)), (top_own, cols(1)), (top_own, cols(2)),
             (low_other, col(0, 0)), (low_other, col(1, 0)), (top_other, col(1, 0)), (top_other, col(2, 0)))
        image_own = image_rows(0)
        value = eye(tile) - diag_tiles(image_own, 0, 1)
        store_packed(pd0, 0, value)
        put(d_refs, own, col(1, 0), value)
        for slot in (0, 2):
            value = -diag_tiles(image_own, 0, slot)
            d0[own, col(slot, 0)] = value
            put(d_refs, own, col(slot, 0), value)
        u_diag = [remote(pd0.at[pl.ds(0, 80)], qdn0.at[pl.ds(0, 80)], "u")]
        d_diag = [remote(pd0.at[pl.ds(0, 80)], qup0.at[pl.ds(0, 80)], "d")]
        u_edge = [remote(d0.at[own, col(2, 0)], d0.at[low_own, col(1, 0)], "u")]
        d_edge = [remote(d0.at[own, col(0, 0)], d0.at[top_own, col(1, 0)], "d")]
        sn[other, col(1, 1)] = load_packed(sx, 0)
        load(sn, s_refs, (other, col(1, 1)), (other, col(2, 1)))
        load(z0, z_refs, (other, col(0, 1)), (other, col(2, 1)))

        x_z[1].wait_recv()
        u_z1 = remote(z0.at[other, col(1, 1)], z0.at[low_other, col(0, 1)], "u")
        d_z1 = remote(z0.at[other, col(1, 1)], z0.at[top_other, col(2, 1)], "d")
        start([u_z1] + u_diag + u_edge, [d_z1] + d_diag + d_edge)
        load(z0, z_refs, (other, col(1, 1)))
        receive([u_z2, u_s2, u_s1], [d_z0, d_s1])
        load(z0, z_refs, (low_other, col(1, 1)), (top_other, col(1, 1)))
        sn[other, col(0, 1)] = sx_dn[...].T
        sn[low_other, col(0, 1)] = load_packed(spx_dn, 0)
        sn[top_other, col(2, 1)] = load_packed(spx_up, 0)
        load(sn, s_refs, (other, col(0, 1)), (low_other, col(0, 1)), (top_other, col(2, 1)))
        image_other = image_rows(1)

        def other_rows(slot):
            return sum(nn(image_other[f], near(z_refs, f, slot)) for f in range(3) if abs(f - slot) < 2)

        cross = -diag_tiles(image_own, 1, 1)
        low_part = jnp.concatenate([jnp.zeros((tile, tile), F32), eye(tile)], axis=1) - other_rows(1)
        pd0[pl.ds(80, tile), :] = cross
        store_packed(pd0, 80 + tile, low_part[:, tile:])
        rest = pl.ds(80, tile + 80)
        u_diag.append(remote(pd0.at[rest], qdn0.at[rest], "u"))
        d_diag.append(remote(pd0.at[rest], qup0.at[rest], "d"))
        start(u_diag[1:], d_diag[1:])
        put(d_refs, own, col(1, 1), cross)
        put(d_refs, other, cols(1), low_part)
        part = {}
        for slot in (2, 0):
            part[slot] = (nn(half_cols(image_own[1], 1), pick(z_refs, other, col(slot, 1))),
                          nn(image_other[1], near(z_refs, 1, slot)))
        receive([u_z1], [d_z1])
        load(z0, z_refs, (low_other, col(0, 1)), (top_other, col(2, 1)))
        edges = {}
        for slot, rows in ((2, top_other), (0, low_other)):
            cross = -(part[slot][0] + nn(half_cols(image_own[slot], 1), pick(z_refs, rows, col(slot, 1))))
            low_part = -(part[slot][1] + nn(image_other[slot], near(z_refs, slot, slot)))
            d0[own, col(slot, 1)] = cross
            d0[other, cols(slot)] = low_part
            edges[slot] = cross, low_part
        u_edge.append(remote(d0.at[own, col(2, 1)], d0.at[low_own, col(1, 1)], "u"))
        u_edge.append(remote(d0.at[other, cols(2)], d0.at[low_other, cols(1)], "u"))
        d_edge.append(remote(d0.at[own, col(0, 1)], d0.at[top_own, col(1, 1)], "d"))
        d_edge.append(remote(d0.at[other, cols(0)], d0.at[top_other, cols(1)], "d"))
        start(u_edge[1:], d_edge[1:])
        for slot in (2, 0):
            put(d_refs, own, col(slot, 1), edges[slot][0])
            put(d_refs, other, cols(slot), edges[slot][1])

        for step in range(ITERS):
            last = step == ITERS - 1
            z, d = (z0, d0) if step == 0 else (z1, d1)
            pd, q_dn, q_up = (pd0, qdn0, qup0) if step == 0 else (pd1, qdn1, qup1)

            if step > 0:
                mid = split(z[row1, cols(1)].T)
                t_own = [nn(mid, near(s_refs, 1, 0)), nt(mid, near(s_refs, 1, 1)), nn(mid, near(s_refs, 1, 2))]
                receive(*edge)
                load_split(z, z_refs, ((0, 1), (2, 1)))
                lower = split(z[row0, cols(1)].T)
                upper = split(z[row2, cols(1)].T)
                t = [
                    split(t_own[0] + nn(lower, near(s_refs, 0, 0))),
                    split(t_own[1] + nt(lower, near(s_refs, 1, 0)) + nt(upper, near(s_refs, 1, 2))),
                    split(t_own[2] + nn(upper, near(s_refs, 2, 2))),
                ]
                value = eye(B) - (nn(t[0], near(z_refs, 0, 1)) + nn(t[1], near(z_refs, 1, 1)) + nn(t[2], near(z_refs, 2, 1)))
                store_packed(pd, 0, value[:tile, :tile])
                pd[pl.ds(80, tile), :] = value[:tile, tile:]
                store_packed(pd, 80 + tile, value[tile:, tile:])
                u_diag, d_diag = [remote(pd, q_dn, "u")], [remote(pd, q_up, "d")]
                start(u_diag, d_diag)
                keep_split(d_refs, 1, 1, value)

                part_up, part_dn = nn(t[1], near(z_refs, 1, 2)), nn(t[1], near(z_refs, 1, 0))
                receive(ups, dns)
                load_split(z, z_refs, ((0, 0), (2, 2)))
                value_up = -(part_up + nn(t[2], near(z_refs, 2, 2)))
                value_dn = -(part_dn + nn(t[0], near(z_refs, 0, 0)))
                d[row1, cols(2)] = value_up
                d[row1, cols(0)] = value_dn
                u_edge = [remote(d.at[row1, cols(2)], d.at[row0, cols(1)], "u")]
                d_edge = [remote(d.at[row1, cols(0)], d.at[row2, cols(1)], "d")]
                start(u_edge, d_edge)
                keep_split(d_refs, 1, 2, value_up)
                keep_split(d_refs, 1, 0, value_dn)

            mine = own if last else row1
            left = [pick(z_refs, mine, cols(k)) for k in range(3)]
            first = [None, None, None]
            first[1] = sum(nt(left[k], near(d_refs, 1, k)) for k in range(3))
            f_mid = split(first[1])
            second_mid = nt(f_mid, near(d_refs, 1, 1))
            receive(u_diag, d_diag)
            for row, ref in ((0, q_dn), (2, q_up)):
                cross = ref[pl.ds(80, tile), :]
                top = jnp.concatenate([load_packed(ref, 0), cross], axis=1)
                low = jnp.concatenate([cross.T, load_packed(ref, 80 + tile)], axis=1)
                keep_split(d_refs, row, row, jnp.concatenate([top, low], axis=0))
            first[0] = nt(left[0], near(d_refs, 0, 0))
            first[2] = nt(left[2], near(d_refs, 2, 2))
            if step == 0:
                x_k.wait_recv()

            def finish(slot, second):
                value = z[mine, cols(slot)] + 0.5 * first[slot] + 0.375 * second
                for g in range(2):
                    part = value[:tile, g * tile:(g + 1) * tile]
                    if not (slot == 1 and g == 0):
                        part = part * keep_own[2 * slot + g]
                    if last:
                        out_ref[:, pl.ds(pl.multiple_of((2 * slot + half_of(g)) * tile, tile), tile)] = part
                        continue
                    z1[own, col(slot, g)] = part
                    part = value[tile:, g * tile:(g + 1) * tile]
                    if not (slot == 1 and g == 1):
                        r = 2 * slot + 1 - g
                        part = part * kx[r:r + 1, :]
                    z1[other, col(slot, g)] = part

            receive(u_edge, d_edge)
            load_split(d, d_refs, ((0, 1), (2, 1)))
            first[0] = first[0] + nt(left[1], near(d_refs, 0, 1))
            first[2] = first[2] + nt(left[1], near(d_refs, 2, 1))
            f_low, f_high = split(first[0]), split(first[2])
            finish(0, nt(f_low, near(d_refs, 0, 0)) + nt(f_mid, near(d_refs, 0, 1)))
            finish(2, nt(f_high, near(d_refs, 2, 2)) + nt(f_mid, near(d_refs, 2, 1)))
            edge = [[], []]
            if not last:
                edge[0].append(remote(z1.at[row1, cols(2)], z1.at[row0, cols(1)], "u"))
                edge[1].append(remote(z1.at[row1, cols(0)], z1.at[row2, cols(1)], "d"))
                start(*edge)
            finish(1, second_mid + nt(f_low, near(d_refs, 1, 0)) + nt(f_high, near(d_refs, 1, 2)))
            if not last:
                ups = [remote(z1.at[row1, cols(1)], z1.at[row0, cols(0)], "u")]
                dns = [remote(z1.at[row1, cols(1)], z1.at[row2, cols(2)], "d")]
                start(ups, dns)
                load_split(z1, z_refs, ((1, 0), (1, 1), (1, 2)))

        for c, where in used:
            if where == "x":
                c.wait_send()

        @pl.when(has_up)
        def _():
            for c, where in used:
                if where == "u":
                    c.wait_send()

        @pl.when(has_dn)
        def _():
            for c, where in used:
                if where == "d":
                    c.wait_send()

    return kernel


def solution(mesh):
    n_blk = mesh.shape["blk"]

    def per_device(intersect, half_factors, z_pattern):
        tile = intersect.shape[0]
        near = pltpu.VMEM((3 * B, 3 * B), F32)
        half = pltpu.VMEM((3 * B, 3 * B), BF16)
        block = pltpu.VMEM((tile, tile), F32)
        packed = pltpu.VMEM((80, tile), F32)
        message = pltpu.VMEM((160 + tile, tile), F32)
        return pl.pallas_call(
            make_kernel(n_blk, tile),
            out_shape=jax.ShapeDtypeStruct(intersect.shape, F32),
            in_specs=[
                pl.BlockSpec(memory_space=pltpu.HBM),
                pl.BlockSpec(memory_space=pltpu.HBM),
                pl.BlockSpec(memory_space=pltpu.HBM),
            ],
            out_specs=pl.BlockSpec(memory_space=pltpu.VMEM),
            scratch_shapes=[near] * 5 + [block] * 3 + [packed] * 6 + [message] * 6 + [pltpu.VMEM((8, tile), F32)] * 2 + [half] * 6

            + [pltpu.SMEM((1, 6), jnp.int32), pltpu.SemaphoreType.DMA((10,)), pltpu.SemaphoreType.DMA((48,)), pltpu.SemaphoreType.DMA((48,))],
            compiler_params=pltpu.CompilerParams(
                collective_id=0, has_side_effects=True, vmem_limit_bytes=48 * 1024 * 1024),
            name="merge",
        )(intersect, half_factors, z_pattern)

    spec = P(("pair", "side", "blk"), None)
    return jax.shard_map(per_device, mesh=mesh, in_specs=(spec,) * 3, out_specs=spec, check_vma=False)
```

```python
import jax
import jax.numpy as jnp
from jax import lax
from jax.experimental import pallas as pl
from jax.experimental.pallas import tpu as pltpu
from jax.sharding import PartitionSpec as P

ITERS = 2
MESH = pl.DeviceIdType.MESH
F32 = jnp.float32
BF16 = jnp.bfloat16
B = 256


def split(value):
    high = value.astype(BF16)
    low = (value - high.astype(F32)).astype(BF16)
    return high, low


def lanes(shape):
    return lax.broadcasted_iota(jnp.int32, shape, 1)


def store_packed(ref, start, tile):
    ref[pl.ds(start, 32), :] = tile[0:32]
    ref[pl.ds(start + 32, 32), :] = jnp.where(lanes((32, 128)) < 32, pltpu.roll(tile[96:128], 32, 1), tile[32:64])
    ref[pl.ds(start + 64, 16), :] = jnp.where(lanes((16, 128)) < 64, pltpu.roll(tile[80:96], 64, 1), tile[64:80])


def load_packed(ref, start):
    first = ref[pl.ds(start, 32), :]
    second = ref[pl.ds(start + 32, 32), :]
    third = ref[pl.ds(start + 64, 16), :]
    upper = jnp.concatenate(
        [first, second, third, pltpu.roll(third, 64, 1), pltpu.roll(second, 96, 1)], axis=0)
    row = lax.broadcasted_iota(jnp.int32, (128, 128), 0)
    return jnp.where(lanes((128, 128)) >= row, upper, upper.T)


def dot3(left, right, nt):
    dims = (((1,), (1 if nt else 0,)), ((), ()))

    def one(x, y):
        return lax.dot_general(x, y, dims, preferred_element_type=F32)

    return one(left[0], right[0]) + one(left[0], right[1]) + one(left[1], right[0])


def make_kernel(n_blk, tile):
    own = pl.ds(B, tile)
    other = pl.ds(B + tile, tile)
    row0, row1, row2 = pl.ds(0, B), pl.ds(B, B), pl.ds(2 * B, B)
    rows_of = (row0, row1, row2)
    low_own, low_other = pl.ds(0, tile), pl.ds(tile, tile)
    top_own, top_other = pl.ds(2 * B, tile), pl.ds(2 * B + tile, tile)

    def col(slot, half):
        return pl.ds(slot * B + half * tile, tile)

    def cols(slot):
        return pl.ds(slot * B, B)

    def kernel(s_hbm, h_hbm, zp_hbm, out_ref, sn, z0, z1, d0, d1, so_dn, so_up, sx_dn, sp, sx, spo_dn, spo_up, spx_dn, spx_up,
               pd0, pd1, qdn0, qdn1, qup0, qup1, kbuf, kx,
               s_hi, s_lo, z_hi, z_lo, d_hi, d_lo, zp_ref, lsem, ssem, rsem):
        side = lax.axis_index("side")
        blk = lax.axis_index("blk")
        partner = {"side": 1 - side}
        up = {"blk": blk + 1}
        dn = {"blk": blk - 1}
        has_up = blk < n_blk - 1
        has_dn = blk > 0

        barrier = pltpu.get_barrier_semaphore()
        pl.semaphore_signal(barrier, inc=1, device_id=partner, device_id_type=MESH)

        @pl.when(has_up)
        def _():
            pl.semaphore_signal(barrier, inc=1, device_id=up, device_id_type=MESH)

        @pl.when(has_dn)
        def _():
            pl.semaphore_signal(barrier, inc=1, device_id=dn, device_id_type=MESH)

        def half_of(g):
            return side if g == 0 else 1 - side

        h_loads = [
            pltpu.make_async_copy(h_hbm.at[:, pl.ds(e * tile, tile)], z0.at[own, col(e, 0)], lsem.at[6 + e])
            for e in range(3)
        ]
        s_loads = []
        for e in range(3):
            for g in range(2):
                src = s_hbm.at[:, pl.ds(pl.multiple_of((2 * e + half_of(g)) * tile, tile), tile)]
                s_loads.append(pltpu.make_async_copy(src, sn.at[own, col(e, g)], lsem.at[2 * e + g]))
        zp_load = pltpu.make_async_copy(zp_hbm, zp_ref, lsem.at[9])
        for load in h_loads + s_loads + [zp_load]:
            load.start()
        for load in h_loads + s_loads:
            load.wait()

        inner = jnp.logical_and(has_up, has_dn)

        @pl.when(inner)
        def _():
            pl.semaphore_wait(barrier, 3)

        @pl.when(jnp.logical_not(inner))
        def _():
            pl.semaphore_wait(barrier, 2)

        used = []

        def remote(src, dst, where):
            i = len(used)
            copy = pltpu.make_async_remote_copy(
                src_ref=src, dst_ref=dst, send_sem=ssem.at[i], recv_sem=rsem.at[i],
                device_id={"x": partner, "u": up, "d": dn}[where], device_id_type=MESH)
            used.append((copy, where))
            return copy

        def start(ups, dns):
            if ups:
                @pl.when(has_up)
                def _():
                    for c in ups:
                        c.start()
            if dns:
                @pl.when(has_dn)
                def _():
                    for c in dns:
                        c.start()

        def receive(ups, dns):
            if ups:
                @pl.when(has_dn)
                def _():
                    for c in ups:
                        c.wait_recv()
            if dns:
                @pl.when(has_up)
                def _():
                    for c in dns:
                        c.wait_recv()

        x_z = [remote(z0.at[own, col(e, 0)], z0.at[other, col(e, 1)], "x") for e in range(3)]
        x_s1 = remote(sp, sx, "x")
        x_s2 = remote(sn.at[own, col(2, 0)], sn.at[other, col(2, 1)], "x")
        x_k = remote(kbuf, kx, "x")
        store_packed(sp, 0, sn[own, col(1, 0)])
        for c in (x_z[0], x_z[2], x_s2):
            c.start()

        u_own = [
            remote(z0.at[own, col(2, 0)], z0.at[low_own, col(1, 0)], "u"),
            remote(sp, spo_dn, "u"),
            remote(sn.at[own, col(1, 1)], sn.at[low_own, col(0, 1)], "u"),
            remote(sn.at[own, col(2, 1)], so_dn, "u"),
            remote(z0.at[own, col(1, 0)], z0.at[low_own, col(0, 0)], "u"),
        ]
        d_own = [
            remote(z0.at[own, col(0, 0)], z0.at[top_own, col(1, 0)], "d"),
            remote(sp, spo_up, "d"),
            remote(sn.at[own, col(1, 1)], sn.at[top_own, col(2, 1)], "d"),
            remote(sn.at[own, col(0, 1)], so_up, "d"),
            remote(z0.at[own, col(1, 0)], z0.at[top_own, col(2, 0)], "d"),
        ]
        start(u_own, d_own)
        for c in (x_s1, x_z[1]):
            c.start()

        zp_load.wait()
        keep_own = [zp_ref[0, 2 * e + half_of(g)].astype(F32) for e in range(3) for g in range(2)]
        row_id = lax.broadcasted_iota(jnp.int32, (8, tile), 0)
        packed = jnp.zeros((8, tile), F32)
        for r in range(6):
            packed = jnp.where(row_id == r, keep_own[r], packed)
        kbuf[...] = packed

        zero = jnp.zeros((tile, tile), F32)
        for e in range(3):
            z0[own, col(e, 1)] = zero
            z0[other, col(e, 0)] = zero
        for e in (0, 1):
            z0[low_own, col(e, 1)] = zero
            z0[low_other, col(e, 0)] = zero
            z0[top_own, col(e + 1, 1)] = zero
            z0[top_other, col(e + 1, 0)] = zero

        @pl.when(jnp.logical_not(has_dn))
        def _():
            for e in (0, 1):
                z0[low_own, col(e, 0)] = zero
                z0[low_other, col(e, 1)] = zero
                z1[row0, cols(e)] = jnp.zeros((B, B), F32)
            for ref in (d0, d1):
                ref[row0, cols(1)] = jnp.zeros((B, B), F32)
            for ref in (spo_dn, spx_dn, qdn0, qdn1):
                ref[...] = jnp.zeros(ref.shape, F32)
            sn[low_own, col(0, 1)] = zero
            so_dn[...] = zero
            sx_dn[...] = zero

        @pl.when(jnp.logical_not(has_up))
        def _():
            for e in (1, 2):
                z0[top_own, col(e, 0)] = zero
                z0[top_other, col(e, 1)] = zero
                z1[row2, cols(e)] = jnp.zeros((B, B), F32)
            for ref in (d0, d1):
                ref[row2, cols(1)] = jnp.zeros((B, B), F32)
            for ref in (spo_up, spx_up, qup0, qup1):
                ref[...] = jnp.zeros(ref.shape, F32)
            sn[top_own, col(2, 1)] = zero
            so_up[...] = zero

        x_k.start()

        s_refs, z_refs, d_refs = (s_hi, s_lo), (z_hi, z_lo), (d_hi, d_lo)

        def keep_split(refs, row, slot, value):
            high, low = split(value)
            refs[0][rows_of[row], cols(slot)] = high
            refs[1][rows_of[row], cols(slot)] = low

        def load_split(ref, refs, places):
            for row, slot in places:
                keep_split(refs, row, slot, ref[rows_of[row], cols(slot)])

        def pick(refs, rows, columns):
            return refs[0][rows, columns], refs[1][rows, columns]

        def near(refs, row, slot):
            return pick(refs, rows_of[row], cols(slot))

        def nn(left, right):
            return dot3(left, right, False)

        def nt(left, right):
            return dot3(left, right, True)

        low_rows, mid_rows, top_rows = (low_own, low_other), (own, other), (top_own, top_other)

        def load(ref, refs, *places):
            for rows, columns in places:
                high, low = split(ref[rows, columns])
                refs[0][rows, columns] = high
                refs[1][rows, columns] = low

        def put(refs, rows, columns, value):
            high, low = split(value)
            refs[0][rows, columns] = high
            refs[1][rows, columns] = low

        def eye(n):
            return (lax.broadcasted_iota(jnp.int32, (n, n), 0) == lax.broadcasted_iota(jnp.int32, (n, n), 1)).astype(F32)

        def image_rows(h):
            mid = split(z0[mid_rows[h], col(1, h)].T)
            lower = split(z0[low_rows[h], col(1, h)].T)
            upper = split(z0[top_rows[h], col(1, h)].T)
            here = [pick(s_refs, mid_rows[h], cols(k)) for k in range(3)]
            return [
                split(nn(lower, pick(s_refs, low_rows[h], cols(0))) + nn(mid, here[0])),
                split(nt(lower, pick(s_refs, row1, col(0, h))) + nn(mid, here[1]) + nt(upper, pick(s_refs, row1, col(2, h)))),
                split(nn(mid, here[2]) + nn(upper, pick(s_refs, top_rows[h], cols(2)))),
            ]

        def half_cols(pair, h):
            return pair[0][:, h * tile:(h + 1) * tile], pair[1][:, h * tile:(h + 1) * tile]

        def diag_tiles(image, h, slot):
            near_rows = (low_rows[h], mid_rows[h], top_rows[h])
            return sum(nn(half_cols(image[f], h), pick(z_refs, near_rows[f], col(slot, h)))
                       for f in range(3) if abs(f - slot) < 2)

        sn[other, col(1, 0)] = sn[own, col(1, 1)].T
        load(sn, s_refs, (own, cols(0)), (own, cols(1)), (own, cols(2)), (other, col(1, 0)))
        load(z0, z_refs, *[(own, cols(e)) for e in range(3)], *[(other, col(e, 0)) for e in range(3)])
        x_z[0].wait_recv()
        d_z0 = remote(z0.at[other, col(0, 1)], z0.at[top_other, col(1, 1)], "d")
        start([], [d_z0])
        x_z[2].wait_recv()
        u_z2 = remote(z0.at[other, col(2, 1)], z0.at[low_other, col(1, 1)], "u")
        start([u_z2], [])
        x_s2.wait_recv()
        u_s2 = remote(sn.at[other, col(2, 1)], sx_dn, "u")
        start([u_s2], [])
        x_s1.wait_recv()
        u_s1 = remote(sx, spx_dn, "u")
        d_s1 = remote(sx, spx_up, "d")
        start([u_s1], [d_s1])

        receive(u_own, d_own)
        sn[other, col(0, 0)] = so_dn[...].T
        sn[other, col(2, 0)] = so_up[...].T
        sn[low_own, col(0, 0)] = load_packed(spo_dn, 0)
        sn[top_own, col(2, 0)] = load_packed(spo_up, 0)
        sn[low_other, col(0, 0)] = sn[low_own, col(0, 1)].T
        sn[top_other, col(2, 0)] = sn[top_own, col(2, 1)].T
        load(sn, s_refs, (low_own, cols(0)), (top_own, cols(2)), (other, col(0, 0)), (other, col(2, 0)),
             (low_other, col(0, 0)), (top_other, col(2, 0)))
        load(z0, z_refs, (low_own, cols(0)), (low_own, cols(1)), (top_own, cols(1)), (top_own, cols(2)),
             (low_other, col(0, 0)), (low_other, col(1, 0)), (top_other, col(1, 0)), (top_other, col(2, 0)))
        image_own = image_rows(0)
        value = eye(tile) - diag_tiles(image_own, 0, 1)
        store_packed(pd0, 0, value)
        put(d_refs, own, col(1, 0), value)
        for slot in (0, 2):
            value = -diag_tiles(image_own, 0, slot)
            d0[own, col(slot, 0)] = value
            put(d_refs, own, col(slot, 0), value)
        u_diag = [remote(pd0.at[pl.ds(0, 80)], qdn0.at[pl.ds(0, 80)], "u")]
        d_diag = [remote(pd0.at[pl.ds(0, 80)], qup0.at[pl.ds(0, 80)], "d")]
        u_edge = [remote(d0.at[own, col(2, 0)], d0.at[low_own, col(1, 0)], "u")]
        d_edge = [remote(d0.at[own, col(0, 0)], d0.at[top_own, col(1, 0)], "d")]
        start(u_diag + u_edge, d_diag + d_edge)
        sn[other, col(1, 1)] = load_packed(sx, 0)
        load(sn, s_refs, (other, col(1, 1)), (other, col(2, 1)))
        load(z0, z_refs, (other, col(0, 1)), (other, col(2, 1)))

        x_z[1].wait_recv()
        u_z1 = remote(z0.at[other, col(1, 1)], z0.at[low_other, col(0, 1)], "u")
        d_z1 = remote(z0.at[other, col(1, 1)], z0.at[top_other, col(2, 1)], "d")
        start([u_z1], [d_z1])
        load(z0, z_refs, (other, col(1, 1)))
        receive([u_z2, u_s2, u_s1], [d_z0, d_s1])
        load(z0, z_refs, (low_other, col(1, 1)), (top_other, col(1, 1)))
        sn[other, col(0, 1)] = sx_dn[...].T
        sn[low_other, col(0, 1)] = load_packed(spx_dn, 0)
        sn[top_other, col(2, 1)] = load_packed(spx_up, 0)
        load(sn, s_refs, (other, col(0, 1)), (low_other, col(0, 1)), (top_other, col(2, 1)))
        image_other = image_rows(1)

        def other_rows(slot):
            return sum(nn(image_other[f], near(z_refs, f, slot)) for f in range(3) if abs(f - slot) < 2)

        cross = -diag_tiles(image_own, 1, 1)
        low_part = jnp.concatenate([jnp.zeros((tile, tile), F32), eye(tile)], axis=1) - other_rows(1)
        pd0[pl.ds(80, tile), :] = cross
        store_packed(pd0, 80 + tile, low_part[:, tile:])
        rest = pl.ds(80, tile + 80)
        u_diag.append(remote(pd0.at[rest], qdn0.at[rest], "u"))
        d_diag.append(remote(pd0.at[rest], qup0.at[rest], "d"))
        start(u_diag[1:], d_diag[1:])
        put(d_refs, own, col(1, 1), cross)
        put(d_refs, other, cols(1), low_part)
        part = {}
        for slot in (2, 0):
            part[slot] = (nn(half_cols(image_own[1], 1), pick(z_refs, other, col(slot, 1))),
                          nn(image_other[1], near(z_refs, 1, slot)))
        receive([u_z1], [d_z1])
        load(z0, z_refs, (low_other, col(0, 1)), (top_other, col(2, 1)))
        edges = {}
        for slot, rows in ((2, top_other), (0, low_other)):
            cross = -(part[slot][0] + nn(half_cols(image_own[slot], 1), pick(z_refs, rows, col(slot, 1))))
            low_part = -(part[slot][1] + nn(image_other[slot], near(z_refs, slot, slot)))
            d0[own, col(slot, 1)] = cross
            d0[other, cols(slot)] = low_part
            edges[slot] = cross, low_part
        u_edge.append(remote(d0.at[own, col(2, 1)], d0.at[low_own, col(1, 1)], "u"))
        u_edge.append(remote(d0.at[other, cols(2)], d0.at[low_other, cols(1)], "u"))
        d_edge.append(remote(d0.at[own, col(0, 1)], d0.at[top_own, col(1, 1)], "d"))
        d_edge.append(remote(d0.at[other, cols(0)], d0.at[top_other, cols(1)], "d"))
        start(u_edge[1:], d_edge[1:])
        for slot in (2, 0):
            put(d_refs, own, col(slot, 1), edges[slot][0])
            put(d_refs, other, cols(slot), edges[slot][1])

        for step in range(ITERS):
            last = step == ITERS - 1
            z, d = (z0, d0) if step == 0 else (z1, d1)
            pd, q_dn, q_up = (pd0, qdn0, qup0) if step == 0 else (pd1, qdn1, qup1)

            if step > 0:
                mid = split(z[row1, cols(1)].T)
                t_own = [nn(mid, near(s_refs, 1, 0)), nt(mid, near(s_refs, 1, 1)), nn(mid, near(s_refs, 1, 2))]
                receive(*edge)
                load_split(z, z_refs, ((0, 1), (2, 1)))
                lower = split(z[row0, cols(1)].T)
                upper = split(z[row2, cols(1)].T)
                t = [
                    split(t_own[0] + nn(lower, near(s_refs, 0, 0))),
                    split(t_own[1] + nt(lower, near(s_refs, 1, 0)) + nt(upper, near(s_refs, 1, 2))),
                    split(t_own[2] + nn(upper, near(s_refs, 2, 2))),
                ]
                value = eye(B) - (nn(t[0], near(z_refs, 0, 1)) + nn(t[1], near(z_refs, 1, 1)) + nn(t[2], near(z_refs, 2, 1)))
                store_packed(pd, 0, value[:tile, :tile])
                pd[pl.ds(80, tile), :] = value[:tile, tile:]
                store_packed(pd, 80 + tile, value[tile:, tile:])
                u_diag, d_diag = [remote(pd, q_dn, "u")], [remote(pd, q_up, "d")]
                start(u_diag, d_diag)
                keep_split(d_refs, 1, 1, value)

                part_up, part_dn = nn(t[1], near(z_refs, 1, 2)), nn(t[1], near(z_refs, 1, 0))
                receive(ups, dns)
                load_split(z, z_refs, ((0, 0), (2, 2)))
                value_up = -(part_up + nn(t[2], near(z_refs, 2, 2)))
                value_dn = -(part_dn + nn(t[0], near(z_refs, 0, 0)))
                d[row1, cols(2)] = value_up
                d[row1, cols(0)] = value_dn
                u_edge = [remote(d.at[row1, cols(2)], d.at[row0, cols(1)], "u")]
                d_edge = [remote(d.at[row1, cols(0)], d.at[row2, cols(1)], "d")]
                start(u_edge, d_edge)
                keep_split(d_refs, 1, 2, value_up)
                keep_split(d_refs, 1, 0, value_dn)

            mine = own if last else row1
            left = [pick(z_refs, mine, cols(k)) for k in range(3)]
            first = [None, None, None]
            first[1] = sum(nt(left[k], near(d_refs, 1, k)) for k in range(3))
            f_mid = split(first[1])
            second_mid = nt(f_mid, near(d_refs, 1, 1))
            receive(u_diag, d_diag)
            for row, ref in ((0, q_dn), (2, q_up)):
                cross = ref[pl.ds(80, tile), :]
                top = jnp.concatenate([load_packed(ref, 0), cross], axis=1)
                low = jnp.concatenate([cross.T, load_packed(ref, 80 + tile)], axis=1)
                keep_split(d_refs, row, row, jnp.concatenate([top, low], axis=0))
            first[0] = nn(left[0], near(d_refs, 0, 0))
            first[2] = nn(left[2], near(d_refs, 2, 2))
            if step == 0:
                x_k.wait_recv()

            def finish(slot, second):
                value = z[mine, cols(slot)] + 0.5 * first[slot] + 0.375 * second
                for g in range(2):
                    part = value[:tile, g * tile:(g + 1) * tile]
                    if not (slot == 1 and g == 0):
                        part = part * keep_own[2 * slot + g]
                    if last:
                        out_ref[:, pl.ds(pl.multiple_of((2 * slot + half_of(g)) * tile, tile), tile)] = part
                        continue
                    z1[own, col(slot, g)] = part
                    part = value[tile:, g * tile:(g + 1) * tile]
                    if not (slot == 1 and g == 1):
                        r = 2 * slot + 1 - g
                        part = part * kx[r:r + 1, :]
                    z1[other, col(slot, g)] = part

            receive(u_edge, d_edge)
            load_split(d, d_refs, ((0, 1), (2, 1)))
            first[0] = first[0] + nt(left[1], near(d_refs, 0, 1))
            first[2] = first[2] + nt(left[1], near(d_refs, 2, 1))
            f_low, f_high = split(first[0]), split(first[2])
            finish(0, nn(f_low, near(d_refs, 0, 0)) + nt(f_mid, near(d_refs, 0, 1)))
            finish(2, nn(f_high, near(d_refs, 2, 2)) + nt(f_mid, near(d_refs, 2, 1)))
            edge = [[], []]
            if not last:
                edge[0].append(remote(z1.at[row1, cols(2)], z1.at[row0, cols(1)], "u"))
                edge[1].append(remote(z1.at[row1, cols(0)], z1.at[row2, cols(1)], "d"))
                start(*edge)
            finish(1, second_mid + nt(f_low, near(d_refs, 1, 0)) + nt(f_high, near(d_refs, 1, 2)))
            if not last:
                ups = [remote(z1.at[row1, cols(1)], z1.at[row0, cols(0)], "u")]
                dns = [remote(z1.at[row1, cols(1)], z1.at[row2, cols(2)], "d")]
                start(ups, dns)
                load_split(z1, z_refs, ((1, 0), (1, 1), (1, 2)))

        for c, where in used:
            if where == "x":
                c.wait_send()

        @pl.when(has_up)
        def _():
            for c, where in used:
                if where == "u":
                    c.wait_send()

        @pl.when(has_dn)
        def _():
            for c, where in used:
                if where == "d":
                    c.wait_send()

    return kernel


def solution(mesh):
    n_blk = mesh.shape["blk"]

    def per_device(intersect, half_factors, z_pattern):
        tile = intersect.shape[0]
        near = pltpu.VMEM((3 * B, 3 * B), F32)
        half = pltpu.VMEM((3 * B, 3 * B), BF16)
        block = pltpu.VMEM((tile, tile), F32)
        packed = pltpu.VMEM((80, tile), F32)
        message = pltpu.VMEM((160 + tile, tile), F32)
        return pl.pallas_call(
            make_kernel(n_blk, tile),
            out_shape=jax.ShapeDtypeStruct(intersect.shape, F32),
            in_specs=[
                pl.BlockSpec(memory_space=pltpu.HBM),
                pl.BlockSpec(memory_space=pltpu.HBM),
                pl.BlockSpec(memory_space=pltpu.HBM),
            ],
            out_specs=pl.BlockSpec(memory_space=pltpu.VMEM),
            scratch_shapes=[near] * 5 + [block] * 3 + [packed] * 6 + [message] * 6 + [pltpu.VMEM((8, tile), F32)] * 2 + [half] * 6

            + [pltpu.SMEM((1, 6), jnp.int32), pltpu.SemaphoreType.DMA((10,)), pltpu.SemaphoreType.DMA((48,)), pltpu.SemaphoreType.DMA((48,))],
            compiler_params=pltpu.CompilerParams(
                collective_id=0, has_side_effects=True, vmem_limit_bytes=48 * 1024 * 1024),
            name="merge",
        )(intersect, half_factors, z_pattern)

    spec = P(("pair", "side", "blk"), None)
    return jax.shard_map(per_device, mesh=mesh, in_specs=(spec,) * 3, out_specs=spec, check_vma=False)
```
